32 devices in a mesh: wide: 8 (over z, y), narrow: 4 (over x, core).
Axes of the slice: x: 2, y: 2, z: 4, core: 2. Of those that a mesh axis runs over, the one named last changes fastest.
Arguments:
- superheat_excess: float32 [32, 512, 512], P('wide', 'narrow'), may hold values from -6 to 6
- liquid_indicator: int32 [32, 512, 512], P('wide', 'narrow'), may hold values from 0 to 1, as said below
- group_patch_listing_table: int32 [8, 4, 16], P('wide', 'narrow'), may hold values from -1 to 31, as said below
- source_smearing_factors_north: float32 [16, 16], replicated, may hold values from 0 to 2, as said below
- source_smearing_factors_east: float32 [128, 128], replicated, may hold values from 0 to 2, as said below
Outputs:
- temperature_next: float32 [32, 512, 512], P('wide', 'narrow')
- pressure: float32 [32, 512, 512], P('wide', 'narrow')
- residual: float32 [32, 512, 512], P('wide', 'narrow')
The draws below stay inside these ranges and needn't reach their ends.
Inputs may be any that keep to these rules, and one draw needn't show every extreme that they name: In each row group_patch_listing_table[w, n] the listed tile numbers come first and are distinct, the remaining entries are -1. A row lists 1 to 16 tiles; for every w the rows n < 4 list exactly 32 tiles together, and one of them lists 16. `liquid_indicator`: phase is 1 in every cell outside the listed tiles. `source_smearing_factors_north`: the identity plus entries drawn in 0 to 1.2 / 16. `source_smearing_factors_east`: the identity plus entries drawn in 0 to 1.2 / 128.
All inputs are finite; a program needn't handle non-finite values.
Results may differ from the reference program's by a relative error of at most 0.0003.
Values sent between devices are 32-bit elements; how exact they have to be, the bound alone decides.
No kernel may reach another device: no remote copies, remote signals or barrier semaphores. Data moves between devices by JAX's collectives and lax.ppermute only.
A program may use at most 64 MiB of HBM per device.

```python
import math
import jax
import jax.numpy as jnp
from jax import lax

MESH_SPAN_EAST = 512
MESH_SPAN_NORTH = 512
CZ = 4
TY = 16
TX = 128
ITERS = 3
MESH_SPAN_UPWARD = 32
NYD = 128
TPD = 32
MAXT = 16
N_WIDE = 8
N_NARROW = 4


def tile_layout(key):
    base = jax.random.fold_in(key, 4242)
    heavy_key, split_key, order_key, coin_key = jax.random.split(base, 4)
    heaviest = jax.random.randint(heavy_key, (N_WIDE,), 0, N_NARROW)

    def light_counts(subkey):
        picks = jax.random.permutation(subkey, MAXT - 1)[:N_NARROW - 2].astype(jnp.int32) + 1
        edges = jnp.concatenate([jnp.zeros((1,), jnp.int32), jnp.sort(picks), jnp.full((1,), MAXT, jnp.int32)])
        return edges[1:] - edges[:-1]
    lighter = jax.vmap(light_counts)(jax.random.split(split_key, N_WIDE))
    lanes = jnp.arange(N_NARROW, dtype=jnp.int32)[None, :]
    others = jnp.clip(lanes - (lanes > heaviest[:, None]).astype(jnp.int32), 0, N_NARROW - 2)
    counts = jnp.where(lanes == heaviest[:, None], MAXT, jnp.take_along_axis(lighter, others, axis=1))
    orders = jax.vmap(lambda subkey: jax.random.permutation(subkey, TPD))(jax.random.split(order_key, N_WIDE * N_NARROW))
    orders = orders.reshape(N_WIDE, N_NARROW, TPD)[:, :, :MAXT].astype(jnp.int32)
    places = jnp.arange(MAXT, dtype=jnp.int32)
    listing = jnp.where(places[None, None, :] < counts[:, :, None], orders, -1).astype(jnp.int32)
    flags = jnp.any(listing[:, :, :, None] == jnp.arange(TPD, dtype=jnp.int32)[None, None, None, :], axis=2)
    return (listing, flags, coin_key)


def draw_liquid_indicator(key, part):
    listing, flags, coin_key = tile_layout(key)
    coins = jax.random.randint(coin_key, (MESH_SPAN_UPWARD, MESH_SPAN_NORTH, MESH_SPAN_EAST), 0, 2)
    tiles_y = NYD // TY
    tiles_x = MESH_SPAN_EAST // TX
    marked = flags.reshape(N_WIDE, 1, N_NARROW, tiles_y, 1, tiles_x, 1)
    marked = jnp.broadcast_to(marked, (N_WIDE, CZ, N_NARROW, tiles_y, TY, tiles_x, TX)).reshape(MESH_SPAN_UPWARD, MESH_SPAN_NORTH, MESH_SPAN_EAST)
    return jnp.where(marked, coins, 1).astype(jnp.int32)


def draw_group_patch_listing_table(key, part):
    return tile_layout(key)[0]


def draw_source_smearing_factors_north(key, part):
    spread = jax.random.uniform(jax.random.fold_in(key, 31), (TY, TY), jnp.float32, 0.0, 1.2 / TY)
    return jnp.eye(TY, dtype=jnp.float32) + spread


def draw_source_smearing_factors_east(key, part):
    spread = jax.random.uniform(jax.random.fold_in(key, 37), (TX, TX), jnp.float32, 0.0, 1.2 / TX)
    return jnp.eye(TX, dtype=jnp.float32) + spread


def level_of(key, shape, cuts, smallest, largest):
    def one(position, parts):
        steps = jax.random.uniform(jax.random.fold_in(jax.random.fold_in(key, 6), position), (parts,), jnp.float32, smallest / len(cuts), largest / len(cuts))
        return jnp.repeat(jnp.exp(steps), shape[position] // parts).reshape((-1,) + (1,) * (len(shape) - position - 1))

    gain = one(*cuts[0])
    for cut in cuts[1:]:
        gain = gain * one(*cut)
    return gain


def gaussian(key, shape, width, reach, cuts=(), kind=jnp.bfloat16):
    entries = jax.random.normal(key, shape, jnp.float32) * width
    if len(cuts) > 0:
        entries = level_of(key, shape, cuts, -0.22, 0.18) * entries
    return jnp.clip(entries, min=-reach, max=reach).astype(kind)


def setup_inputs(seed: int = 0) -> dict:
    streams_of = jax.random.split(jax.random.key(seed), 6)
    superheat_excess = gaussian(streams_of[0], (MESH_SPAN_UPWARD, MESH_SPAN_NORTH, MESH_SPAN_EAST), 1.0, 6.0, ((0, 8), (1, 4)), jnp.float32)
    liquid_indicator = draw_liquid_indicator(jax.random.fold_in(streams_of[5], 71), 0)
    group_patch_listing_table = draw_group_patch_listing_table(jax.random.fold_in(streams_of[5], 71), 0)
    source_smearing_factors_north = draw_source_smearing_factors_north(jax.random.fold_in(streams_of[5], 71), 0)
    source_smearing_factors_east = draw_source_smearing_factors_east(jax.random.fold_in(streams_of[5], 71), 0)
    return {"superheat_excess": superheat_excess, "liquid_indicator": liquid_indicator, "group_patch_listing_table": group_patch_listing_table, "source_smearing_factors_north": source_smearing_factors_north, "source_smearing_factors_east": source_smearing_factors_east}


conduct_liquid = 1.0
conduct_vapor = 0.4
diffusion = 0.06
mobility_liquid = 1.0
mobility_vapor = 4.0
expansion = 0.3
compress = 0.01
highest = lax.Precision.HIGHEST

def centre(padded):
    return padded[1:-1, 1:-1, 1:-1]

def neighbours(padded):
    return [padded[2:, 1:-1, 1:-1], padded[:-2, 1:-1, 1:-1], padded[1:-1, 2:, 1:-1], padded[1:-1, :-2, 1:-1], padded[1:-1, 1:-1, 2:], padded[1:-1, 1:-1, :-2]]

def heat_advance(temp_pad, liquid_indicator_haloed, inner_region_haloed):
    current = centre(temp_pad)
    phases = centre(liquid_indicator_haloed)
    conduct = jnp.where(phases > 0.5, conduct_liquid, conduct_vapor)
    flux = jnp.zeros_like(current)
    faces = jnp.zeros_like(current)
    for near_temp, near_phase, near_inside in zip(neighbours(temp_pad), neighbours(liquid_indicator_haloed), neighbours(inner_region_haloed)):
        differ = jnp.abs(near_phase - phases) > 0.5
        flux = flux + near_inside * jnp.where(differ, -2.0 * current, near_temp - current)
        faces = faces + near_inside * jnp.where(differ, 1.0, 0.0)
    heated_values = current + diffusion * conduct * flux
    vaporised_amount = 2.0 * conduct * faces * heated_values
    return (heated_values, vaporised_amount)

def face_weights(liquid_indicator_haloed, inner_region_haloed):
    mobility = jnp.where(liquid_indicator_haloed > 0.5, mobility_liquid, mobility_vapor)
    own = centre(mobility)
    return [near_inside * 0.5 * (own + near_mob) for near_inside, near_mob in zip(neighbours(inner_region_haloed), neighbours(mobility))]

def apply_operator(field_pad, weights):
    field = centre(field_pad)
    total = compress * field
    for weight, near in zip(weights, neighbours(field_pad)):
        total = total + weight * (field - near)
    return total

def smear_tiles(tiles, source_smearing_factors_north, source_smearing_factors_east):
    across = jnp.einsum('...bc,dc->...bd', tiles, source_smearing_factors_east, precision=highest)
    return expansion * jnp.einsum('ab,...bd->...ad', source_smearing_factors_north, across, precision=highest)

def cosine_rows(extent, kfirst, klength, cfirst, clength):
    waves = kfirst + jnp.arange(klength, dtype=jnp.int32)
    centres = 2 * (cfirst + jnp.arange(clength, dtype=jnp.int32)) + 1
    turns = waves[:, None] * centres[None, :] % (4 * extent)
    angles = 2.0 * math.pi / (4 * extent) * turns.astype(jnp.float32)
    scales = jnp.where(waves == 0, math.sqrt(1.0 / extent), math.sqrt(2.0 / extent)).astype(jnp.float32)
    return scales[:, None] * jnp.cos(angles)

def eigen(extent, first, length):
    waves = (first + jnp.arange(length, dtype=jnp.int32)).astype(jnp.float32)
    return 4.0 * jnp.sin(waves * (math.pi / (2 * extent))) ** 2

def tile_source(vaporised_amount, group_patch_listing_table, source_smearing_factors_north, source_smearing_factors_east):
    size_y = source_smearing_factors_north.shape[0]
    size_x = source_smearing_factors_east.shape[0]
    tiles_y = MESH_SPAN_NORTH // N_NARROW // size_y
    tiles_x = MESH_SPAN_EAST // size_x
    blocks = vaporised_amount.reshape(N_WIDE, CZ, N_NARROW, tiles_y, size_y, tiles_x, size_x)
    blocks = blocks.transpose(0, 2, 3, 5, 1, 4, 6).reshape(N_WIDE, N_NARROW, tiles_y * tiles_x, CZ, size_y, size_x)
    numbers = jnp.arange(tiles_y * tiles_x, dtype=jnp.int32)
    listed = jnp.any(group_patch_listing_table[:, :, :, None] == numbers[None, None, None, :], axis=2)
    smeared = smear_tiles(blocks, source_smearing_factors_north, source_smearing_factors_east) * listed[:, :, :, None, None, None].astype(jnp.float32)
    smeared = smeared.reshape(N_WIDE, N_NARROW, tiles_y, tiles_x, CZ, size_y, size_x)
    return smeared.transpose(0, 4, 1, 2, 5, 3, 6).reshape(MESH_SPAN_UPWARD, MESH_SPAN_NORTH, MESH_SPAN_EAST)

def precondition(remainder):
    table_x = cosine_rows(MESH_SPAN_EAST, 0, MESH_SPAN_EAST, 0, MESH_SPAN_EAST)
    table_y = cosine_rows(MESH_SPAN_NORTH, 0, MESH_SPAN_NORTH, 0, MESH_SPAN_NORTH)
    table_z = cosine_rows(MESH_SPAN_UPWARD, 0, MESH_SPAN_UPWARD, 0, MESH_SPAN_UPWARD)
    spectrum = jnp.einsum('zyx,kx->zyk', remainder, table_x, precision=highest)
    spectrum = jnp.einsum('zyk,ly->zlk', spectrum, table_y, precision=highest)
    spectrum = jnp.einsum('zlk,mz->mlk', spectrum, table_z, precision=highest)
    denom = eigen(MESH_SPAN_UPWARD, 0, MESH_SPAN_UPWARD)[:, None, None] + eigen(MESH_SPAN_NORTH, 0, MESH_SPAN_NORTH)[None, :, None] + eigen(MESH_SPAN_EAST, 0, MESH_SPAN_EAST)[None, None, :] + compress
    spectrum = spectrum / denom
    spectrum = jnp.einsum('mlk,mz->zlk', spectrum, table_z, precision=highest)
    spectrum = jnp.einsum('zlk,ly->zyk', spectrum, table_y, precision=highest)
    return jnp.einsum('zyk,kx->zyx', spectrum, table_x, precision=highest)

def reference(superheat_excess, liquid_indicator, group_patch_listing_table, source_smearing_factors_north, source_smearing_factors_east):
    liquid_indicator_haloed = jnp.pad(liquid_indicator.astype(jnp.float32), 1)
    inner_region_haloed = jnp.pad(jnp.ones(liquid_indicator.shape, jnp.float32), 1)
    heated_values, vaporised_amount = heat_advance(jnp.pad(superheat_excess, 1), liquid_indicator_haloed, inner_region_haloed)
    source = tile_source(vaporised_amount, group_patch_listing_table, source_smearing_factors_north, source_smearing_factors_east)
    weights = face_weights(liquid_indicator_haloed, inner_region_haloed)
    pressure = jnp.zeros_like(source)
    residual = source
    search = precondition(residual)
    aligned = jnp.sum(residual * search)
    direction = search
    for iteration in range(ITERS):
        image = apply_operator(jnp.pad(direction, 1), weights)
        alpha = aligned / jnp.sum(direction * image)
        pressure = pressure + alpha * direction
        residual = residual - alpha * image
        if iteration + 1 < ITERS:
            search = precondition(residual)
            renewed = jnp.sum(residual * search)
            direction = search + renewed / aligned * direction
            aligned = renewed
    return (heated_values, pressure, residual)
```

```python
import math

import jax
import jax.numpy as jnp
import numpy as np
from jax import lax
from jax.experimental import pallas as pl
from jax.experimental.pallas import tpu as pltpu
from jax.sharding import PartitionSpec as P

ITERS = 3

conduct_liquid = 1.0
conduct_vapor = 0.4
diffusion = 0.06
mobility_liquid = 1.0
mobility_vapor = 4.0
expansion = 0.3
compress = 0.01
highest = lax.Precision.HIGHEST
f32 = jnp.float32
LANES = 128
VMEM = pltpu.VMEM
ORDER = ("narrow", "wide")


def mat(a, b):
    return lax.dot_general(
        a, b, (((1,), (0,)), ((), ())), precision=highest, preferred_element_type=f32
    )


def mat_t(a, b):
    return lax.dot_general(
        a, b, (((1,), (1,)), ((), ())), precision=highest, preferred_element_type=f32
    )


def cosine(m):
    k = np.arange(m)[:, None]
    i = np.arange(m)[None, :]
    scale = np.where(k == 0, math.sqrt(1.0 / m), math.sqrt(2.0 / m))
    return scale * np.cos(np.pi * (k * (2 * i + 1) % (4 * m)) / (2 * m))


def eigen(m):
    return 4.0 * np.sin(np.pi * np.arange(m) / (2 * m)) ** 2


def tables(depth, rows, span, blocks):
    half = depth // 2
    c_z, c_r, c_x = cosine(depth), cosine(rows), cosine(span)
    order = np.concatenate([np.arange(0, depth, 2), np.arange(1, depth, 2)])
    forward = []
    for parity in range(2):
        c = c_z[parity::2, :half]
        forward.append(
            np.einsum("ky,mz->kmzy", c_r, c).reshape(rows * half, half * rows)
        )
    c_sorted = c_z[order]
    swap = np.zeros((2 * depth, 2 * depth))
    swap[:depth, :depth] = c_sorted.T
    swap[depth:, depth:] = c_sorted.T
    shift = eigen(depth)[order][:, None] + eigen(span)[None, :] + compress
    lam = eigen(rows)
    first, last = c_r[:, 0], c_r[:, rows - 1]
    den = lam[None, :, None] + shift[:, None, :]
    same = ((first**2)[None, :, None] / den).sum(1)
    cross = ((first * last)[None, :, None] / den).sum(1)
    m = np.arange(1, blocks)
    sine = np.zeros((blocks, blocks))
    sine[: blocks - 1, : blocks - 1] = math.sqrt(2.0 / blocks) * np.sin(
        np.pi * m[:, None] * m[None, :] / blocks
    )
    wave = np.zeros((blocks, 1))
    wave[: blocks - 1, 0] = 2.0 * np.cos(np.pi * m / blocks)
    return {
        "c_x": c_x.astype(np.float32),
        "forward": np.stack(forward).astype(np.float32),
        "inverse": np.stack([f.T for f in forward]).astype(np.float32),
        "swap": swap.astype(np.float32),
        "shift": shift.astype(np.float32),
        "lam": [float(v) for v in lam],
        "first": [float(v) for v in first],
        "last": [float(v) for v in last],
        "pair": np.stack([1.0 + 2.0 * same, cross], 1).astype(np.float32),
        "sine": sine.astype(np.float32),
        "wave": np.broadcast_to(wave, (blocks, LANES)).astype(np.float32).copy(),
    }


def call(body, outs, *args, smem=(), scratch=(), flops=1e9, name=None):
    specs = [
        pl.BlockSpec(memory_space=pltpu.SMEM if i in smem else VMEM) for i in range(len(args))
    ]
    return pl.pallas_call(
        body,
        out_shape=[jax.ShapeDtypeStruct(s, f32) for s in outs],
        in_specs=specs,
        out_specs=[pl.BlockSpec(memory_space=VMEM)] * len(outs),
        scratch_shapes=list(scratch),
        compiler_params=pltpu.CompilerParams(vmem_limit_bytes=40 * 2**20),
        cost_estimate=pl.CostEstimate(flops=int(flops), bytes_accessed=4 << 20, transcendentals=0),
        name=name,
    )(*args)


def step(count, aligned, body):
    if aligned:
        lax.fori_loop(0, count, lambda i, c: (body(i), c)[1], 0)
    else:
        for i in range(count):
            body(i)


def row_roll(x, up):
    n = x.shape[0]
    if n % 8 == 0:
        return pltpu.roll(x, n - 1 if up else 1, 0)
    if up:
        return jnp.concatenate([x[1:], x[:1]], 0)
    return jnp.concatenate([x[-1:], x[:-1]], 0)


def lane_roll(x, up):
    n = x.shape[1]
    return pltpu.roll(x, n - 1 if up else 1, 1)


def fold_lanes(x):
    total = x[:, :LANES]
    for i in range(1, x.shape[1] // LANES):
        total = total + x[:, i * LANES : (i + 1) * LANES]
    return jnp.sum(total, axis=0, keepdims=True)


def heat_body(dims, *refs):
    thick, north, span, size_y, size_x, most = dims
    (pos, table, temp, phase, zlo, zhi, ylo, yhi, smear_n, smear_e,
     heated, source, tp, pp, mass, mask) = refs
    tiles_y = north // size_y
    tiles_x = span // size_x
    w_first, w_last = pos[0] == 0, pos[1] == 0
    n_first, n_last = pos[2] == 0, pos[3] == 0
    for z in range(thick):
        tp[z + 1] = temp[z]
        pp[z + 1] = phase[z].astype(f32)
    tp[0] = jnp.where(w_first, temp[0], zlo[0])
    pp[0] = jnp.where(w_first, phase[0].astype(f32), zlo[1])
    tp[thick + 1] = jnp.where(w_last, temp[thick - 1], zhi[0])
    pp[thick + 1] = jnp.where(w_last, phase[thick - 1].astype(f32), zhi[1])
    row = lax.broadcasted_iota(jnp.int32, (tiles_y, span), 0)
    lane = lax.broadcasted_iota(jnp.int32, (tiles_y, span), 1)
    tile = row * tiles_x + lane // size_x
    hit = tile == table[0]
    for i in range(1, most):
        hit = jnp.logical_or(hit, tile == table[i])
    mask[...] = jnp.where(hit, expansion, 0.0)
    r = lax.broadcasted_iota(jnp.int32, (size_y, span), 0)
    c = lax.broadcasted_iota(jnp.int32, (size_y, span), 1)

    def plane(z):
        for yc in range(tiles_y):
            at = pl.ds(yc * size_y, size_y)
            t = tp[z + 1, at, :]
            p = pp[z + 1, at, :]

            def edge(ref, halo, k, y, wall, own):
                if 0 <= y < north:
                    return ref[z + 1, pl.ds(y, 1), :]
                return jnp.where(wall, own, halo[k, z])

            pairs = [
                (tp[z, at, :], pp[z, at, :]),
                (tp[z + 2, at, :], pp[z + 2, at, :]),
                (jnp.where(c == span - 1, t, lane_roll(t, True)),
                 jnp.where(c == span - 1, p, lane_roll(p, True))),
                (jnp.where(c == 0, t, lane_roll(t, False)),
                 jnp.where(c == 0, p, lane_roll(p, False))),
            ]
            y = (yc + 1) * size_y
            pairs.append((
                jnp.where(r == size_y - 1, edge(tp, yhi, 0, y, n_last, t[size_y - 1:]), row_roll(t, True)),
                jnp.where(r == size_y - 1, edge(pp, yhi, 1, y, n_last, p[size_y - 1:]), row_roll(p, True)),
            ))
            y = yc * size_y - 1
            pairs.append((
                jnp.where(r == 0, edge(tp, ylo, 0, y, n_first, t[:1]), row_roll(t, False)),
                jnp.where(r == 0, edge(pp, ylo, 1, y, n_first, p[:1]), row_roll(p, False)),
            ))
            flux = jnp.zeros_like(t)
            faces = jnp.zeros_like(t)
            for near_t, near_p in pairs:
                differ = near_p != p
                flux = flux + jnp.where(differ, -2.0 * t, near_t - t)
                faces = faces + jnp.where(differ, 1.0, 0.0)
            k = jnp.where(p > 0.5, conduct_liquid, conduct_vapor)
            value = t + diffusion * k * flux
            heated[z, at, :] = value
            mass[pl.ds(pl.multiple_of(z * north, north) + yc * size_y, size_y), :] = 2.0 * k * faces * value

    lax.fori_loop(0, thick, lambda z, carry: (plane(z), carry)[1], 0)
    for tx in range(tiles_x):
        at = slice(tx * size_x, (tx + 1) * size_x)
        mass[:, at] = mat_t(mass[:, at], smear_e[...])
    for z in range(thick):
        smeared = mat(smear_n[...], mass[z * north : (z + 1) * north, :])
        for yc in range(tiles_y):
            source[yc, z] = smeared[yc * size_y : (yc + 1) * size_y] * mask[yc : yc + 1, :]


def forward_body(dims, tab, field, fold, spec, fwd, c_x, shift, message, extra):
    depth, rows, span = dims
    half = depth // 2
    size = half * rows
    aligned = rows % 8 == 0
    for parity in range(2):
        for z in range(half):
            a = field[z * rows : (z + 1) * rows, :]
            b = field[(depth - 1 - z) * rows : (depth - z) * rows, :]
            fold[z * rows : (z + 1) * rows, :] = a + b if parity == 0 else a - b
        spec[parity * size : (parity + 1) * size, :] = mat_t(
            mat(fwd[parity], fold[:size, :]), c_x[...]
        )
    for parity in range(2):
        mu = shift[parity * half : (parity + 1) * half, :]
        low = jnp.zeros((half, span), f32)
        high = jnp.zeros((half, span), f32)
        for ky in range(rows):
            at = parity * size + ky * half
            g = spec[at : at + half, :] / (mu + tab["lam"][ky])
            low = low + tab["first"][ky] * g
            high = high + tab["last"][ky] * g
        for k in range(half):
            o = parity * half + k
            message[o, 0:1, :span] = low[k : k + 1]
            message[o, 0:1, span : 2 * span] = high[k : k + 1]
            message[o, 0:1, 2 * span :] = extra


def start_body(dims, tab, source, fwd, c_x, shift, spec, message, fold):
    forward_body(dims, tab, source, fold, spec, fwd, c_x, shift, message, jnp.zeros((1, LANES), f32))


def solve_body(dims, tab, first_call, blocks, *refs):
    depth, rows, span = dims
    half = depth // 2
    if first_call:
        (got, spec, shift, pair, sine, wave, h_new, message, low, high) = refs
    else:
        (got, spec, shift, pair, sine, wave, image_spec, h_old, rho,
         spec_new, h_new, message, alpha_out, low, high) = refs
    for j in range(blocks):
        low[j : j + 1, :] = got[j, 0:1, :span]
        high[j : j + 1, :] = got[j, 0:1, span : 2 * span]
    jump = high[...] - row_roll(low[...], True)
    r = lax.broadcasted_iota(jnp.int32, (blocks, span), 0)
    jump = jnp.where(r == blocks - 1, 0.0, jump)
    if not first_call:
        bottom = jnp.zeros((1, LANES), f32)
        for j in range(blocks):
            bottom = bottom + got[j, 0:1, 2 * span :]
        alpha = rho[...] / jnp.sum(bottom, axis=1, keepdims=True)
        alpha_out[...] = alpha
        alpha = alpha[:, :1]
        jump = h_old[...] - alpha * jump
    h_new[...] = jump
    scale = 1.0 / (pair[0:1, :] - wave[:, :1] * pair[1:2, :])
    q = mat(sine[...], mat(sine[...], jump) * scale)
    total = fold_lanes(q * jump) * -1.0
    acc = jnp.zeros((8, span), f32)
    for parity in range(2):
        mu = shift[parity * half : (parity + 1) * half, :]
        for ky in range(rows):
            at = parity * half * rows + ky * half
            s = spec[at : at + half, :]
            if not first_call:
                s = s - alpha * image_spec[at : at + half, :]
                spec_new[at : at + half, :] = s
            e = s * s / (mu + tab["lam"][ky])
            for i in range(half // 8):
                acc = acc + e[i * 8 : (i + 1) * 8]
    total = total + fold_lanes(acc)
    zero = jnp.zeros((1, span), f32)
    for j in range(blocks):
        message[j, 0:1, :span] = zero if j == 0 else q[j - 1 : j]
        message[j, 0:1, span : 2 * span] = q[j : j + 1]
        message[j, 0:1, 2 * span :] = total


def advance_body(dims, tab, first_call, last_call, blocks, *refs):
    depth, rows, span = dims
    half = depth // 2
    size = half * rows
    refs = list(refs)
    take = refs.pop
    got, spec, shift, inv, fwd, c_x, swap, mob, mob_lo, mob_hi = [take(0) for _ in range(10)]
    if not first_call:
        dir_old, q_old, rho_old = [take(0) for _ in range(3)]
    direction, image = take(0), take(0)
    if last_call:
        rho_out, part_out = take(0), take(0)
    else:
        rho_out, dir_spec, q_out, image_spec, message = [take(0) for _ in range(5)]
    work, q_mid, fold = take(0), take(0), take(0)
    if last_call:
        dir_spec, q_out = take(0), take(0)

    total = jnp.zeros((1, LANES), f32)
    for o in range(depth):
        q_mid[o : o + 1, :] = got[o, 0:1, :span]
        q_mid[depth + o : depth + o + 1, :] = got[o, 0:1, span : 2 * span]
        total = total + got[o, 0:1, 2 * span :]
    rho = jnp.sum(total, axis=1, keepdims=True) + jnp.zeros((1, LANES), f32)
    rho_out[...] = rho
    if not first_call:
        beta = (rho / rho_old[...])[:, :1]
    for parity in range(2):
        at_q = parity * half
        mu = shift[at_q : at_q + half, :]
        q_lo = q_mid[at_q : at_q + half, :]
        q_hi = q_mid[depth + at_q : depth + at_q + half, :]
        for ky in range(rows):
            at = parity * size + ky * half
            u = (spec[at : at + half, :] + tab["first"][ky] * q_lo - tab["last"][ky] * q_hi) / (
                mu + tab["lam"][ky]
            )
            if not first_call:
                u = u + beta * dir_old[at : at + half, :]
            dir_spec[at : at + half, :] = u
    q = q_mid[...]
    if not first_call:
        q = q + beta * q_old[...]
    q_out[...] = q
    q_mid[...] = mat(swap[...], mat(q, c_x[...]))
    for parity in range(2):
        fold[parity * size : (parity + 1) * size, :] = mat(
            inv[parity], mat(dir_spec[parity * size : (parity + 1) * size, :], c_x[...])
        )
    for z in range(half):
        a = fold[z * rows : (z + 1) * rows, :]
        b = fold[size + z * rows : size + (z + 1) * rows, :]
        direction[z * rows : (z + 1) * rows, :] = a + b
        direction[(depth - 1 - z) * rows : (depth - z) * rows, :] = a - b

    r = lax.broadcasted_iota(jnp.int32, (rows, span), 0)
    c = lax.broadcasted_iota(jnp.int32, (rows, span), 1)
    acc = jnp.zeros((1, span), f32)
    below = None
    for z in range(depth):
        at = slice(z * rows, (z + 1) * rows)
        v = direction[at, :]
        b = mob[at, :]
        out = compress * v
        flux = jnp.where(c == span - 1, 0.0, (b + lane_roll(b, True)) * (v - lane_roll(v, True)))
        out_flux = flux - lane_roll(flux, False)
        b_hi = b[rows - 1 :] + mob_hi[z : z + 1, :]
        flux = jnp.where(
            r == rows - 1,
            b_hi * q_mid[depth + z : depth + z + 1, :],
            (b + row_roll(b, True)) * (v - row_roll(v, True)),
        )
        f_lo = (b[:1] + mob_lo[z : z + 1, :]) * q_mid[z : z + 1, :]
        out_flux = out_flux + flux - jnp.where(r == 0, f_lo, row_roll(flux, False))
        if below is not None:
            out_flux = out_flux - below
        if z + 1 < depth:
            up = slice((z + 1) * rows, (z + 2) * rows)
            below = (b + mob[up, :]) * (v - direction[up, :])
            out_flux = out_flux + below
        out = out + 0.5 * out_flux
        image[at, :] = out
        acc = acc + jnp.sum(v * out, axis=0, keepdims=True)
    part = fold_lanes(acc)
    if last_call:
        for i in range(blocks):
            part_out[i] = part
    else:
        forward_body(dims, tab, image, work, image_spec, fwd, c_x, shift, message, part)


def on_device(superheat_excess, liquid_indicator, listing, smear_n, smear_e):
    thick, north, span = superheat_excess.shape
    wide, lanes = lax.axis_size("wide"), lax.axis_size("narrow")
    w, n = lax.axis_index("wide"), lax.axis_index("narrow")
    blocks = wide * lanes
    depth = thick * wide
    rows = north // wide
    size_y, size_x = smear_n.shape[0], smear_e.shape[0]
    tiles_y = north // size_y
    dims = (depth, rows, span)
    tab = tables(depth, rows, span, blocks)
    own = n * wide + w
    whole = depth * rows

    phase = liquid_indicator.astype(f32)
    both = jnp.stack([superheat_excess, phase])
    up = [(i, i + 1) for i in range(wide - 1)]
    down = [(i + 1, i) for i in range(wide - 1)]
    zlo = lax.ppermute(both[:, thick - 1], "wide", up)
    zhi = lax.ppermute(both[:, 0], "wide", down)
    up = [(i, i + 1) for i in range(lanes - 1)]
    down = [(i + 1, i) for i in range(lanes - 1)]
    ylo = lax.ppermute(both[:, :, north - 1 :], "narrow", up)
    yhi = lax.ppermute(both[:, :, :1], "narrow", down)

    def regroup(x):
        x = x.reshape(wide, thick * rows, span)
        return lax.all_to_all(x, "wide", split_axis=0, concat_axis=0, tiled=True)

    mob = jnp.where(phase > 0.5, mobility_liquid, mobility_vapor)
    mob = mob.reshape(thick, wide, rows, span).transpose(1, 0, 2, 3)
    mob = regroup(mob).reshape(depth, rows, span)

    def place(j):
        return (j % wide) * lanes + j // wide

    up = [(place(j), place(j + 1)) for j in range(blocks - 1)]
    down = [(b, a) for a, b in up]
    mob_lo = lax.ppermute(mob[:, rows - 1], ("wide", "narrow"), up)
    mob_hi = lax.ppermute(mob[:, 0], ("wide", "narrow"), down)
    mob = mob.reshape(whole, span)

    pos = jnp.stack([w, wide - 1 - w, n, lanes - 1 - n]).astype(jnp.int32)
    blockn = (jnp.eye(tiles_y, dtype=f32)[:, None, :, None] * smear_n[None, :, None, :]).reshape(
        north, north
    )
    most = listing.size
    heat_dims = (thick, north, span, size_y, size_x, most)
    heated, source = call(
        lambda *r: heat_body(heat_dims, *r),
        [(thick, north, span), (tiles_y, thick, size_y, span)],
        pos, listing.reshape(-1), superheat_excess, liquid_indicator, zlo, zhi, ylo, yhi, blockn, smear_e,
        smem=(0, 1),
        scratch=[
            VMEM((thick + 2, north, span), f32),
            VMEM((thick + 2, north, span), f32),
            VMEM((thick * north, span), f32),
            VMEM((tiles_y, span), f32),
        ],
        name="heat",
    )
    if size_y != rows:
        source = source.transpose(1, 0, 2, 3).reshape(thick, wide, rows, span).transpose(1, 0, 2, 3)
    source = regroup(source).reshape(whole, span)

    c_x, fwd, inv = (jnp.asarray(tab[k]) for k in ("c_x", "forward", "inverse"))
    swap, shift, sine, wave = (jnp.asarray(tab[k]) for k in ("swap", "shift", "sine", "wave"))
    pair = lax.dynamic_index_in_dim(jnp.asarray(tab["pair"]), own, 0, keepdims=False)
    full = (whole, span)
    letter = (blocks, 1, 2 * span + LANES)
    one = (1, LANES)

    def swap_all(x):
        return lax.all_to_all(x, ORDER, split_axis=0, concat_axis=0, tiled=True)

    spec, message = call(
        lambda *r: start_body(dims, tab, *r), [full, letter], source, fwd, c_x, shift,
        scratch=[VMEM(full, f32)], name="start",
    )
    pair_scratch = [VMEM((blocks, span), f32)] * 2
    jump, message = call(
        lambda *r: solve_body(dims, tab, True, blocks, *r), [(blocks, span), letter],
        swap_all(message), spec, shift, pair, sine, wave, scratch=pair_scratch, name="solve",
    )
    pressure, residual = None, source
    dir_spec = q = rho = None
    for iteration in range(ITERS):
        first, final = iteration == 0, iteration + 1 == ITERS
        args = [swap_all(message), spec, shift, inv, fwd, c_x, swap, mob, mob_lo, mob_hi]
        if not first:
            args += [dir_spec, q, rho]
        outs = [full, full, one]
        work = [VMEM(full, f32), VMEM((2 * depth, span), f32), VMEM(full, f32)]
        if final:
            outs += [(blocks, 1, LANES)]
            work += [VMEM(full, f32), VMEM((2 * depth, span), f32)]
        else:
            outs += [full, (2 * depth, span), full, letter]
        result = call(
            lambda *r, a=first, b=final: advance_body(dims, tab, a, b, blocks, *r), outs, *args,
            scratch=work, name="advance",
        )
        direction, image, rho = result[:3]
        if final:
            bottom = jnp.sum(swap_all(result[3]))
            alpha = rho[0, 0] / bottom
        else:
            dir_spec, q, image_spec, message = result[3:]
            spec, jump, message, alpha = call(
                lambda *r: solve_body(dims, tab, False, blocks, *r),
                [full, (blocks, span), letter, one],
                swap_all(message), spec, shift, pair, sine, wave, image_spec, jump, rho,
                scratch=pair_scratch, name="solve",
            )
            alpha = alpha[0, 0]
        pressure = alpha * direction if first else pressure + alpha * direction
        residual = residual - alpha * image

    both = jnp.stack([pressure, residual]).reshape(2, wide, thick, rows, span)
    both = lax.all_to_all(both, "wide", split_axis=1, concat_axis=1, tiled=True)
    both = both.transpose(0, 2, 1, 3, 4).reshape(2, thick, north, span)
    return heated, both[0], both[1]


def solution(mesh):
    spec = P("wide", "narrow", None)
    return jax.shard_map(
        on_device,
        mesh=mesh,
        in_specs=(spec, spec, spec, P(), P()),
        out_specs=(spec, spec, spec),
        check_vma=False,
    )
```

```python
import math

import jax
import jax.numpy as jnp
import numpy as np
from jax import lax
from jax.experimental import pallas as pl
from jax.experimental.pallas import tpu as pltpu
from jax.sharding import PartitionSpec as P

ITERS = 3

conduct_liquid = 1.0
conduct_vapor = 0.4
diffusion = 0.06
mobility_liquid = 1.0
mobility_vapor = 4.0
expansion = 0.3
compress = 0.01
highest = lax.Precision.HIGHEST
f32 = jnp.float32
LANES = 128
VMEM = pltpu.VMEM
ORDER = ("narrow", "wide")


def mat(a, b):
    return lax.dot_general(
        a, b, (((1,), (0,)), ((), ())), precision=highest, preferred_element_type=f32
    )


def mat_t(a, b):
    return lax.dot_general(
        a, b, (((1,), (1,)), ((), ())), precision=highest, preferred_element_type=f32
    )


def cosine(m):
    k = np.arange(m)[:, None]
    i = np.arange(m)[None, :]
    scale = np.where(k == 0, math.sqrt(1.0 / m), math.sqrt(2.0 / m))
    return scale * np.cos(np.pi * (k * (2 * i + 1) % (4 * m)) / (2 * m))


def eigen(m):
    return 4.0 * np.sin(np.pi * np.arange(m) / (2 * m)) ** 2


def tables(depth, rows, span, blocks):
    half = depth // 2
    c_z, c_r, c_x = cosine(depth), cosine(rows), cosine(span)
    order = np.concatenate([np.arange(0, depth, 2), np.arange(1, depth, 2)])
    forward = []
    for parity in range(2):
        c = c_z[parity::2, :half]
        forward.append(
            np.einsum("ky,mz->kmzy", c_r, c).reshape(rows * half, half * rows)
        )
    c_sorted = c_z[order]
    swap = np.zeros((2 * depth, 2 * depth))
    swap[:depth, :depth] = c_sorted.T
    swap[depth:, depth:] = c_sorted.T
    shift = eigen(depth)[order][:, None] + eigen(span)[None, :] + compress
    lam = eigen(rows)
    first, last = c_r[:, 0], c_r[:, rows - 1]
    den = lam[None, :, None] + shift[:, None, :]
    same = ((first**2)[None, :, None] / den).sum(1)
    cross = ((first * last)[None, :, None] / den).sum(1)
    m = np.arange(1, blocks)
    sine = np.zeros((blocks, blocks))
    sine[: blocks - 1, : blocks - 1] = math.sqrt(2.0 / blocks) * np.sin(
        np.pi * m[:, None] * m[None, :] / blocks
    )
    wave = np.zeros((blocks, 1))
    wave[: blocks - 1, 0] = 2.0 * np.cos(np.pi * m / blocks)
    return {
        "c_x": c_x.astype(np.float32),
        "forward": np.stack(forward).astype(np.float32),
        "inverse": np.stack([f.T for f in forward]).astype(np.float32),
        "swap": swap.astype(np.float32),
        "shift": shift.astype(np.float32),
        "lam": [float(v) for v in lam],
        "first": [float(v) for v in first],
        "last": [float(v) for v in last],
        "pair": np.stack([1.0 + 2.0 * same, cross], 1).astype(np.float32),
        "sine": sine.astype(np.float32),
        "wave": np.broadcast_to(wave, (blocks, LANES)).astype(np.float32).copy(),
    }


def call(body, outs, *args, smem=(), far=(), scratch=(), flops=1e9, name=None):
    specs = [
        pl.BlockSpec(memory_space=pltpu.SMEM if i in smem else pl.ANY if i in far else VMEM)
        for i in range(len(args))
    ]
    return pl.pallas_call(
        body,
        out_shape=[jax.ShapeDtypeStruct(s, f32) for s in outs],
        in_specs=specs,
        out_specs=[pl.BlockSpec(memory_space=VMEM)] * len(outs),
        scratch_shapes=list(scratch),
        compiler_params=pltpu.CompilerParams(vmem_limit_bytes=16 * 2**20),
        cost_estimate=pl.CostEstimate(flops=int(flops), bytes_accessed=4 << 20, transcendentals=0),
        name=name,
    )(*args)


def step(count, aligned, body):
    if aligned:
        lax.fori_loop(0, count, lambda i, c: (body(i), c)[1], 0)
    else:
        for i in range(count):
            body(i)


def row_roll(x, up):
    n = x.shape[0]
    if n % 8 == 0:
        return pltpu.roll(x, n - 1 if up else 1, 0)
    if up:
        return jnp.concatenate([x[1:], x[:1]], 0)
    return jnp.concatenate([x[-1:], x[:-1]], 0)


def lane_roll(x, up):
    n = x.shape[1]
    return pltpu.roll(x, n - 1 if up else 1, 1)


def fold_lanes(x):
    total = x[:, :LANES]
    for i in range(1, x.shape[1] // LANES):
        total = total + x[:, i * LANES : (i + 1) * LANES]
    return jnp.sum(total, axis=0, keepdims=True)


def smear_blocks(smear, size):
    n = smear.shape[0]
    i = lax.broadcasted_iota(jnp.int32, (n, size), 0)
    j = lax.broadcasted_iota(jnp.int32, (n, size), 1)
    wide_pick = jnp.where(i == j % n, 1.0, 0.0)
    i = lax.broadcasted_iota(jnp.int32, (size, n), 0)
    j = lax.broadcasted_iota(jnp.int32, (size, n), 1)
    tall_pick = jnp.where(i % n == j, 1.0, 0.0)
    tiled = mat(tall_pick, mat(smear, wide_pick))
    i = lax.broadcasted_iota(jnp.int32, (size, size), 0)
    j = lax.broadcasted_iota(jnp.int32, (size, size), 1)
    return jnp.where(i // n == j // n, tiled, 0.0)


def conducted(t, p, pairs):
    flux = jnp.zeros_like(t)
    faces = jnp.zeros_like(t)
    for near_t, near_p in pairs:
        differ = near_p != p
        flux = flux + jnp.where(differ, -2.0 * t, near_t - t)
        faces = faces + jnp.where(differ, 1.0, 0.0)
    k = jnp.where(p > 0.5, conduct_liquid, conduct_vapor)
    value = t + diffusion * k * flux
    return value, 2.0 * k * faces * value


def heat_body(dims, *refs):
    thick, north, span, size_y, size_x, most = dims
    with_source = most > 0
    if with_source:
        (table, temp, phase, zlo, zhi, ylo, yhi, smear, smear_e,
         heated, source, tp, pp, mass, mask) = refs
    else:
        temp, phase, ylo, yhi, heated, pp = refs
        tp = temp
    base = 1 if with_source else 0
    tiles_y = north // size_y
    tiles_x = span // size_x
    w, n = lax.axis_index("wide"), lax.axis_index("narrow")
    n_first, n_last = n == 0, n == lax.axis_size("narrow") - 1
    for z in range(thick):
        pp[z + base] = phase[z].astype(f32)
    if with_source:
        w_first, w_last = w == 0, w == lax.axis_size("wide") - 1
        for z in range(thick):
            tp[z + 1] = temp[z]
        tp[0] = jnp.where(w_first, temp[0], zlo[0])
        pp[0] = jnp.where(w_first, phase[0].astype(f32), zlo[1])
        tp[thick + 1] = jnp.where(w_last, temp[thick - 1], zhi[0])
        pp[thick + 1] = jnp.where(w_last, phase[thick - 1].astype(f32), zhi[1])
        row = lax.broadcasted_iota(jnp.int32, (tiles_y, span), 0)
        lane = lax.broadcasted_iota(jnp.int32, (tiles_y, span), 1)
        tile = row * tiles_x + lane // size_x
        hit = tile == table[0]
        for i in range(1, most):
            hit = jnp.logical_or(hit, tile == table[i])
        mask[...] = jnp.where(hit, expansion, 0.0)
    r = lax.broadcasted_iota(jnp.int32, (size_y, span), 0)
    c = lax.broadcasted_iota(jnp.int32, (size_y, span), 1)

    def plane(z):
        for yc in range(tiles_y):
            at = pl.ds(yc * size_y, size_y)
            t = tp[z + base, at, :]
            p = pp[z + base, at, :]

            def edge(ref, halo, k, y, wall, own):
                if 0 <= y < north:
                    return ref[z + base, pl.ds(y, 1), :]
                return jnp.where(wall, own, halo[k, z])

            pairs = [
                (tp[z + base - 1, at, :], pp[z + base - 1, at, :]),
                (tp[z + base + 1, at, :], pp[z + base + 1, at, :]),
                (jnp.where(c == span - 1, t, lane_roll(t, True)),
                 jnp.where(c == span - 1, p, lane_roll(p, True))),
                (jnp.where(c == 0, t, lane_roll(t, False)),
                 jnp.where(c == 0, p, lane_roll(p, False))),
            ]
            y = (yc + 1) * size_y
            pairs.append((
                jnp.where(r == size_y - 1, edge(tp, yhi, 0, y, n_last, t[size_y - 1:]), row_roll(t, True)),
                jnp.where(r == size_y - 1, edge(pp, yhi, 1, y, n_last, p[size_y - 1:]), row_roll(p, True)),
            ))
            y = yc * size_y - 1
            pairs.append((
                jnp.where(r == 0, edge(tp, ylo, 0, y, n_first, t[:1]), row_roll(t, False)),
                jnp.where(r == 0, edge(pp, ylo, 1, y, n_first, p[:1]), row_roll(p, False)),
            ))
            value, vapor = conducted(t, p, pairs)
            heated[z if with_source else z - 1, at, :] = value
            if with_source:
                to = pl.ds(pl.multiple_of(z * north, north) + yc * size_y, size_y)
                mass[to, :] = vapor

    inner = 1 - base
    lax.fori_loop(inner, thick - inner, lambda z, carry: (plane(z), carry)[1], 0)
    if not with_source:
        return
    smear_n = smear_blocks(smear[...], north)
    for tx in range(tiles_x):
        at = slice(tx * size_x, (tx + 1) * size_x)
        mass[:, at] = mat_t(mass[:, at], smear_e[...])
    for z in range(thick):
        smeared = mat(smear_n, mass[z * north : (z + 1) * north, :])
        for yc in range(tiles_y):
            source[yc, z] = smeared[yc * size_y : (yc + 1) * size_y] * mask[yc : yc + 1, :]


def pack_body(dims, listing, far_temp, far_phase, out, side_first, side_last, temp, phase, entry, sems):
    wide, thick, rows, span, most = dims
    tiles = span // LANES
    per = thick * tiles * rows
    north = wide * rows
    copies = [
        pltpu.make_async_copy(far_temp, temp, sems.at[0]),
        pltpu.make_async_copy(far_phase, phase, sems.at[1]),
    ]
    for copy in copies:
        copy.start()
    entry[...] = jnp.full((8, LANES), -1.0, f32)
    entry[0:1, 0:most] = listing[0].astype(f32)
    for w in range(wide):
        out[w, 2 * per :, :] = entry[...]
    for a, ref in enumerate((temp, phase)):
        copies[a].wait()
        for z in range(thick):
            side_first[a, z] = ref[z, 0:1, :].astype(f32)
            side_last[a, z] = ref[z, north - 1 : north, :].astype(f32)
            for w in range(wide):
                for t in range(tiles):
                    at = a * per + (z * tiles + t) * rows
                    piece = ref[z, w * rows : (w + 1) * rows, t * LANES : (t + 1) * LANES]
                    out[w, at : at + rows, :] = piece.astype(f32)


def edge_body(dims, got, first, last):
    wide, thick, rows, span, _ = dims
    tiles = span // LANES
    per = thick * tiles * rows
    for a in range(2):
        for w in range(wide):
            for z in range(thick):
                for t in range(tiles):
                    at = a * per + (z * tiles + t) * rows
                    row = a * wide * thick + w * thick + z
                    lanes = slice(t * LANES, (t + 1) * LANES)
                    first[row : row + 1, lanes] = got[w, at : at + 1, :]
                    last[row : row + 1, lanes] = got[w, at + rows - 1 : at + rows, :]


def boil_body(dims, tab, got, lo, hi, smear, smear_e, fwd, c_x, shift,
              source, mob, mob_lo, mob_hi, spec, message, outer, tp, pp, mass, heated, mask, entries):
    wide, thick, rows, span, _ = dims
    depth = wide * thick
    tiles = span // LANES
    per = thick * tiles * rows
    size_x = smear_e.shape[0]
    for w in range(wide):
        entries[w : w + 1, :] = got[w, 2 * per : 2 * per + 1, :]
        for z in range(thick):
            for t in range(tiles):
                at = (z * tiles + t) * rows
                to = ((w * thick + z) * rows, t * LANES)
                to = (slice(to[0], to[0] + rows), slice(to[1], to[1] + LANES))
                tp[to] = got[w, at : at + rows, :]
                pp[to] = got[w, per + at : per + at + rows, :]
    for tx in range(span // size_x):
        tile = (lax.axis_index("wide") * (span // size_x) + tx).astype(f32)
        hit = jnp.where(entries[...] == tile, expansion, 0.0)
        hit = jnp.max(hit, axis=1, keepdims=True)
        mask[:, tx * size_x : (tx + 1) * size_x] = jnp.broadcast_to(hit, (wide, size_x))
    mob[...] = jnp.where(pp[...] > 0.5, mobility_liquid, mobility_vapor)
    mob_lo[...] = jnp.where(lo[depth:, :] > 0.5, mobility_liquid, mobility_vapor)
    mob_hi[...] = jnp.where(hi[depth:, :] > 0.5, mobility_liquid, mobility_vapor)
    r = lax.broadcasted_iota(jnp.int32, (rows, span), 0)
    c = lax.broadcasted_iota(jnp.int32, (rows, span), 1)
    own = lax.axis_index("narrow") * wide + lax.axis_index("wide")
    no_lo, no_hi = own == 0, own == lax.axis_size("narrow") * wide - 1

    def at_z(z):
        return pl.ds(pl.multiple_of(z * rows, rows), rows)

    def slab(z):
        t, p = tp[at_z(z), :], pp[at_z(z), :]
        below, above = at_z(jnp.maximum(z - 1, 0)), at_z(jnp.minimum(z + 1, depth - 1))

        def along_y(x, k, up):
            if up:
                edge = jnp.where(no_hi, x[rows - 1 :], hi[pl.ds(k * depth + z, 1), :])
                return jnp.where(r == rows - 1, edge, row_roll(x, True))
            edge = jnp.where(no_lo, x[:1], lo[pl.ds(k * depth + z, 1), :])
            return jnp.where(r == 0, edge, row_roll(x, False))

        pairs = [
            (tp[below, :], pp[below, :]),
            (tp[above, :], pp[above, :]),
            (along_y(t, 0, True), along_y(p, 1, True)),
            (along_y(t, 0, False), along_y(p, 1, False)),
            (jnp.where(c == span - 1, t, lane_roll(t, True)),
             jnp.where(c == span - 1, p, lane_roll(p, True))),
            (jnp.where(c == 0, t, lane_roll(t, False)),
             jnp.where(c == 0, p, lane_roll(p, False))),
        ]
        heated[at_z(z), :], mass[at_z(z), :] = conducted(t, p, pairs)

    lax.fori_loop(0, depth, lambda z, carry: (slab(z), carry)[1], 0)
    for w in range(wide):
        for k, z in enumerate((w * thick, (w + 1) * thick - 1)):
            outer[w, k * rows : (k + 1) * rows, :] = heated[z * rows : (z + 1) * rows, :]
    for tx in range(span // size_x):
        at = slice(tx * size_x, (tx + 1) * size_x)
        mass[:, at] = mat_t(mass[:, at], smear_e[...])
    group = LANES
    smear_n = smear_blocks(smear[...], group)
    for g in range(depth * rows // group):
        smeared = mat(smear_n, mass[g * group : (g + 1) * group, :])
        for i in range(group // rows):
            z = g * (group // rows) + i
            source[z * rows : (z + 1) * rows, :] = (
                smeared[i * rows : (i + 1) * rows] * mask[z // thick : z // thick + 1, :]
            )
    forward_body(
        (depth, rows, span), tab, source, mass, spec, fwd, c_x, shift, message,
        jnp.zeros((1, LANES), f32),
    )


def finish_body(dims, rho, parts, p, r, d, image, *refs):
    outer, out = refs if len(refs) == 2 else (None, refs[0])
    wide, thick, rows, span, _ = dims
    total = parts[0]
    for i in range(1, parts.shape[0]):
        total = total + parts[i]
    alpha = (rho[...] / jnp.sum(total, axis=1, keepdims=True))[:, :1]
    n = thick * rows
    for w in range(wide):
        at = slice(w * n, (w + 1) * n)
        out[w, :n, :] = p[at, :] + alpha * d[at, :]
        out[w, n : 2 * n, :] = r[at, :] - alpha * image[at, :]
        if outer is not None:
            out[w, 2 * n :, :] = outer[w]


def spread_body(dims, got, *refs):
    wide, thick, rows, span, _ = dims
    inner, outs = (refs[0], refs[1:]) if len(refs) == 4 else (None, refs)
    for k, out in enumerate(outs):
        for z in range(thick):
            row = (k * thick + z) * rows
            if k == 2:
                if 0 < z < thick - 1:
                    out[z] = inner[z - 1]
                    continue
                row = (2 * thick + (z > 0)) * rows
            for w in range(wide):
                out[z, w * rows : (w + 1) * rows, :] = got[w, row : row + rows, :]


def forward_body(dims, tab, field, fold, spec, fwd, c_x, shift, message, extra):
    depth, rows, span = dims
    half = depth // 2
    size = half * rows
    aligned = rows % 8 == 0
    for parity in range(2):
        for z in range(half):
            a = field[z * rows : (z + 1) * rows, :]
            b = field[(depth - 1 - z) * rows : (depth - z) * rows, :]
            fold[z * rows : (z + 1) * rows, :] = a + b if parity == 0 else a - b
        spec[parity * size : (parity + 1) * size, :] = mat_t(
            mat(fwd[parity], fold[:size, :]), c_x[...]
        )
    for parity in range(2):
        mu = shift[parity * half : (parity + 1) * half, :]
        low = jnp.zeros((half, span), f32)
        high = jnp.zeros((half, span), f32)
        for ky in range(rows):
            at = parity * size + ky * half
            g = spec[at : at + half, :] / (mu + tab["lam"][ky])
            low = low + tab["first"][ky] * g
            high = high + tab["last"][ky] * g
        for k in range(half):
            o = parity * half + k
            message[o, 0:1, :span] = low[k : k + 1]
            message[o, 0:1, span : 2 * span] = high[k : k + 1]
            message[o, 0:1, 2 * span :] = extra


def start_body(dims, tab, source, fwd, c_x, shift, spec, message, fold):
    forward_body(dims, tab, source, fold, spec, fwd, c_x, shift, message, jnp.zeros((1, LANES), f32))


def solve_body(dims, tab, first_call, blocks, *refs):
    depth, rows, span = dims
    half = depth // 2
    if first_call:
        (got, spec, shift, pairs, sine, wave, h_new, message, low, high) = refs
    else:
        (got, spec, shift, pairs, sine, wave, image_spec, h_old, rho,
         spec_new, h_new, message, alpha_out, low, high) = refs
    pair = pairs[lax.axis_index("narrow") * lax.axis_size("wide") + lax.axis_index("wide")]
    for j in range(blocks):
        low[j : j + 1, :] = got[j, 0:1, :span]
        high[j : j + 1, :] = got[j, 0:1, span : 2 * span]
    jump = high[...] - row_roll(low[...], True)
    r = lax.broadcasted_iota(jnp.int32, (blocks, span), 0)
    jump = jnp.where(r == blocks - 1, 0.0, jump)
    if not first_call:
        bottom = jnp.zeros((1, LANES), f32)
        for j in range(blocks):
            bottom = bottom + got[j, 0:1, 2 * span :]
        alpha = rho[...] / jnp.sum(bottom, axis=1, keepdims=True)
        alpha_out[...] = alpha
        alpha = alpha[:, :1]
        jump = h_old[...] - alpha * jump
    h_new[...] = jump
    scale = 1.0 / (pair[0:1, :] - wave[:, :1] * pair[1:2, :])
    q = mat(sine[...], mat(sine[...], jump) * scale)
    total = fold_lanes(q * jump) * -1.0
    acc = jnp.zeros((8, span), f32)
    for parity in range(2):
        mu = shift[parity * half : (parity + 1) * half, :]
        for ky in range(rows):
            at = parity * half * rows + ky * half
            s = spec[at : at + half, :]
            if not first_call:
                s = s - alpha * image_spec[at : at + half, :]
                spec_new[at : at + half, :] = s
            e = s * s / (mu + tab["lam"][ky])
            for i in range(half // 8):
                acc = acc + e[i * 8 : (i + 1) * 8]
    total = total + fold_lanes(acc)
    zero = jnp.zeros((1, span), f32)
    for j in range(blocks):
        message[j, 0:1, :span] = zero if j == 0 else q[j - 1 : j]
        message[j, 0:1, span : 2 * span] = q[j : j + 1]
        message[j, 0:1, 2 * span :] = total


def advance_body(dims, tab, first_call, last_call, blocks, *refs):
    depth, rows, span = dims
    half = depth // 2
    size = half * rows
    refs = list(refs)
    take = refs.pop
    if last_call:
        n = ITERS - 1
        at = 13
        refs[at : at + 3 * n] = [refs[at : at + n], refs[at + n : at + 2 * n], refs[at + 2 * n : at + 3 * n]]
    got, spec, shift, inv, fwd, c_x, swap, mob, mob_lo, mob_hi = [take(0) for _ in range(10)]
    if not first_call:
        dir_old, q_old, rho_old = [take(0) for _ in range(3)]
    if last_call:
        alphas, olds, images, source = take(0), take(0), take(0), take(0)
    direction, image = take(0), take(0)
    if last_call:
        rho_out, part_out, p_out, r_out = [take(0) for _ in range(4)]
    else:
        rho_out, dir_spec, q_out, image_spec, message = [take(0) for _ in range(5)]
    work, q_mid, fold = take(0), take(0), take(0)
    if last_call:
        dir_spec, q_out = take(0), take(0)

    total = jnp.zeros((1, LANES), f32)
    for o in range(depth):
        q_mid[o : o + 1, :] = got[o, 0:1, :span]
        q_mid[depth + o : depth + o + 1, :] = got[o, 0:1, span : 2 * span]
        total = total + got[o, 0:1, 2 * span :]
    rho = jnp.sum(total, axis=1, keepdims=True) + jnp.zeros((1, LANES), f32)
    rho_out[...] = rho
    if not first_call:
        beta = (rho / rho_old[...])[:, :1]
    for parity in range(2):
        at_q = parity * half
        mu = shift[at_q : at_q + half, :]
        q_lo = q_mid[at_q : at_q + half, :]
        q_hi = q_mid[depth + at_q : depth + at_q + half, :]
        for ky in range(rows):
            at = parity * size + ky * half
            u = (spec[at : at + half, :] + tab["first"][ky] * q_lo - tab["last"][ky] * q_hi) / (
                mu + tab["lam"][ky]
            )
            if not first_call:
                u = u + beta * dir_old[at : at + half, :]
            dir_spec[at : at + half, :] = u
    q = q_mid[...]
    if not first_call:
        q = q + beta * q_old[...]
    q_out[...] = q
    q_mid[...] = mat(swap[...], mat(q, c_x[...]))
    for parity in range(2):
        fold[parity * size : (parity + 1) * size, :] = mat(
            inv[parity], mat(dir_spec[parity * size : (parity + 1) * size, :], c_x[...])
        )
    for z in range(half):
        a = fold[z * rows : (z + 1) * rows, :]
        b = fold[size + z * rows : size + (z + 1) * rows, :]
        direction[z * rows : (z + 1) * rows, :] = a + b
        direction[(depth - 1 - z) * rows : (depth - z) * rows, :] = a - b

    r = lax.broadcasted_iota(jnp.int32, (rows, span), 0)
    c = lax.broadcasted_iota(jnp.int32, (rows, span), 1)
    acc = jnp.zeros((1, span), f32)
    below = None
    for z in range(depth):
        at = slice(z * rows, (z + 1) * rows)
        v = direction[at, :]
        b = mob[at, :]
        out = compress * v
        flux = jnp.where(c == span - 1, 0.0, (b + lane_roll(b, True)) * (v - lane_roll(v, True)))
        out_flux = flux - lane_roll(flux, False)
        b_hi = b[rows - 1 :] + mob_hi[z : z + 1, :]
        flux = jnp.where(
            r == rows - 1,
            b_hi * q_mid[depth + z : depth + z + 1, :],
            (b + row_roll(b, True)) * (v - row_roll(v, True)),
        )
        f_lo = (b[:1] + mob_lo[z : z + 1, :]) * q_mid[z : z + 1, :]
        out_flux = out_flux + flux - jnp.where(r == 0, f_lo, row_roll(flux, False))
        if below is not None:
            out_flux = out_flux - below
        if z + 1 < depth:
            up = slice((z + 1) * rows, (z + 2) * rows)
            below = (b + mob[up, :]) * (v - direction[up, :])
            out_flux = out_flux + below
        out = out + 0.5 * out_flux
        image[at, :] = out
        acc = acc + jnp.sum(v * out, axis=0, keepdims=True)
    part = fold_lanes(acc)
    if last_call:
        for i in range(blocks):
            part_out[i] = part
        p = alphas[0][:, :1] * olds[0][...]
        r = source[...] - alphas[0][:, :1] * images[0][...]
        for i in range(1, len(olds)):
            p = p + alphas[i][:, :1] * olds[i][...]
            r = r - alphas[i][:, :1] * images[i][...]
        p_out[...] = p
        r_out[...] = r
    else:
        forward_body(dims, tab, image, work, image_spec, fwd, c_x, shift, message, part)


def split_by_z(superheat_excess, liquid_indicator, listing, smear_n, smear_e, dims, const):
    thick, north, span = superheat_excess.shape
    wide, lanes = lax.axis_size("wide"), lax.axis_size("narrow")
    depth, rows, span = dims[1]
    size_y, size_x = smear_n.shape[0], smear_e.shape[0]
    tiles_y = north // size_y
    whole = depth * rows
    phase = liquid_indicator.astype(f32)
    both = jnp.stack([superheat_excess, phase])
    up = [(i, i + 1) for i in range(wide - 1)]
    down = [(i + 1, i) for i in range(wide - 1)]
    zlo = lax.ppermute(both[:, thick - 1], "wide", up)
    zhi = lax.ppermute(both[:, 0], "wide", down)
    up = [(i, i + 1) for i in range(lanes - 1)]
    down = [(i + 1, i) for i in range(lanes - 1)]
    ylo = lax.ppermute(both[:, :, north - 1 :], "narrow", up)
    yhi = lax.ppermute(both[:, :, :1], "narrow", down)

    def regroup(x):
        x = x.reshape(wide, thick * rows, span)
        return lax.all_to_all(x, "wide", split_axis=0, concat_axis=0, tiled=True)

    mob = jnp.where(phase > 0.5, mobility_liquid, mobility_vapor)
    mob = mob.reshape(thick, wide, rows, span).transpose(1, 0, 2, 3)
    mob = regroup(mob).reshape(depth, rows, span)
    most = listing.size
    heat_dims = (thick, north, span, size_y, size_x, most)
    heated, source = call(
        lambda *r: heat_body(heat_dims, *r),
        [(thick, north, span), (tiles_y, thick, size_y, span)],
        listing.reshape(-1), superheat_excess, liquid_indicator, zlo, zhi, ylo, yhi,
        smear_n, smear_e,
        smem=(0,),
        scratch=[
            VMEM((thick + 2, north, span), f32),
            VMEM((thick + 2, north, span), f32),
            VMEM((thick * north, span), f32),
            VMEM((tiles_y, span), f32),
        ],
        name="heat",
    )
    source, mob = lax.optimization_barrier((source, mob))
    if size_y != rows:
        source = source.transpose(1, 0, 2, 3).reshape(thick, wide, rows, span).transpose(1, 0, 2, 3)
    source = regroup(source).reshape(whole, span)
    up, down = const["row_pairs"]
    mob_lo = lax.ppermute(mob[:, rows - 1], ("wide", "narrow"), up)
    mob_hi = lax.ppermute(mob[:, 0], ("wide", "narrow"), down)
    spec, message = call(
        lambda *r: start_body(dims[1], const["tab"], *r), [(whole, span), const["letter"]],
        source, const["forward"], const["c_x"], const["shift"],
        scratch=[VMEM((whole, span), f32)], name="start",
    )
    return heated, source, mob.reshape(whole, span), mob_lo, mob_hi, spec, message


def split_by_y(superheat_excess, liquid_indicator, listing, smear_n, smear_e, dims, const):
    depth, rows, span = dims[1]
    wide, thick = dims[0][:2]
    whole = depth * rows
    per = thick * rows * (span // LANES)
    north = superheat_excess.shape[1]
    packed, side_first, side_last = call(
        lambda *r: pack_body(dims[0], *r),
        [(wide, 2 * per + 8, LANES), (2, thick, 1, span), (2, thick, 1, span)],
        listing, superheat_excess, liquid_indicator, far=(1, 2),
        scratch=[
            VMEM((thick, north, span), f32),
            VMEM((thick, north, span), jnp.int32),
            VMEM((8, LANES), f32),
            pltpu.SemaphoreType.DMA((2,)),
        ],
        name="pack",
    )
    got = lax.all_to_all(packed, "wide", split_axis=0, concat_axis=0, tiled=True)
    first, last = call(lambda *r: edge_body(dims[0], *r), [(2 * depth, span)] * 2, got, name="edge")
    up, down = const["row_pairs"]
    lo = lax.ppermute(last, ("wide", "narrow"), up)
    hi = lax.ppermute(first, ("wide", "narrow"), down)
    full, plane = (whole, span), (depth, span)
    return side_first, side_last, *call(
        lambda *r: boil_body(dims[0], const["tab"], *r),
        [full, full, plane, plane, full, const["letter"], (wide, 2 * rows, span)],
        got, lo, hi, smear_n, smear_e, const["forward"], const["c_x"], const["shift"],
        scratch=[VMEM(full, f32)] * 4 + [VMEM((wide, span), f32), VMEM((wide, LANES), f32)],
        name="boil",
    )


def on_device(superheat_excess, liquid_indicator, listing, smear_n, smear_e):
    thick, north, span = superheat_excess.shape
    wide, lanes = lax.axis_size("wide"), lax.axis_size("narrow")
    blocks = wide * lanes
    depth = thick * wide
    rows = north // wide
    size_y = smear_n.shape[0]
    shape = (depth, rows, span)
    dims = ((wide, thick, rows, span, listing.size), shape)
    tab = tables(depth, rows, span, blocks)
    whole = depth * rows
    full, one = (whole, span), (1, LANES)
    letter = (blocks, 1, 2 * span + LANES)

    def place(j):
        return (j % wide) * lanes + j // wide

    up = [(place(j), place(j + 1)) for j in range(blocks - 1)]
    const = {k: jnp.asarray(tab[k]) for k in ("c_x", "forward", "inverse", "swap", "shift", "pair", "sine", "wave")}
    const["tab"], const["letter"] = tab, letter
    const["row_pairs"] = up, [(b, a) for a, b in up]
    by_y = rows == size_y and thick > 2
    if by_y:
        side_first, side_last, source, mob, mob_lo, mob_hi, spec, message, outer = split_by_y(
            superheat_excess, liquid_indicator, listing, smear_n, smear_e, dims, const
        )
    else:
        heated, source, mob, mob_lo, mob_hi, spec, message = split_by_z(
            superheat_excess, liquid_indicator, listing, smear_n, smear_e, dims, const
        )

    def swap_all(x):
        return lax.all_to_all(x, ORDER, split_axis=0, concat_axis=0, tiled=True)

    shift, pair, sine, wave = (const[k] for k in ("shift", "pair", "sine", "wave"))
    pair_scratch = [VMEM((blocks, span), f32)] * 2
    jump, message = call(
        lambda *r: solve_body(shape, tab, True, blocks, *r), [(blocks, span), letter],
        swap_all(message), spec, shift, pair, sine, wave, scratch=pair_scratch,
        name="solve",
    )
    dir_spec = q = rho = None
    directions, images, alphas = [], [], []
    for iteration in range(ITERS):
        first, final = iteration == 0, iteration + 1 == ITERS
        args = [swap_all(message), spec, shift, const["inverse"], const["forward"], const["c_x"], const["swap"], mob, mob_lo, mob_hi]
        if not first:
            args += [dir_spec, q, rho]
        outs = [full, full, one]
        work = [VMEM(full, f32), VMEM((2 * depth, span), f32), VMEM(full, f32)]
        if final:
            outs += [(blocks, 1, LANES), full, full]
            args += [*alphas, *directions, *images, source]
            work += [VMEM(full, f32), VMEM((2 * depth, span), f32)]
        else:
            outs += [full, (2 * depth, span), full, letter]
        result = call(
            lambda *r, a=first, b=final: advance_body(shape, tab, a, b, blocks, *r), outs, *args,
            scratch=work, name="advance",
        )
        directions.append(result[0])
        images.append(result[1])
        rho = result[2]
        if final:
            parts = swap_all(result[3])
            pressure, residual = result[4:]
        else:
            dir_spec, q, image_spec, message = result[3:]
            spec, jump, message, alpha = call(
                lambda *r: solve_body(shape, tab, False, blocks, *r),
                [full, (blocks, span), letter, one],
                swap_all(message), spec, shift, pair, sine, wave, image_spec, jump, rho,
                scratch=pair_scratch, name="solve",
            )
            alphas.append(alpha)

    extra = [outer] if by_y else []
    (both,) = call(
        lambda *r: finish_body(dims[0], *r), [(wide, 2 * (thick + len(extra)) * rows, span)],
        rho, parts, pressure, residual, directions[2], images[2], *extra, name="finish",
    )
    both = lax.all_to_all(both, "wide", split_axis=0, concat_axis=0, tiled=True)
    outs = [(thick, north, span)] * (2 + len(extra))
    if not by_y:
        pressure, residual = call(
            lambda *r: spread_body(dims[0], *r), outs, both, name="spread"
        )
        return heated, pressure, residual
    y_up = [(i, i + 1) for i in range(lanes - 1)]
    y_down = [(i + 1, i) for i in range(lanes - 1)]
    ylo = lax.ppermute(side_last, "narrow", y_up)
    yhi = lax.ppermute(side_first, "narrow", y_down)
    (inner,) = call(
        lambda *r: heat_body((thick, north, span, size_y, span, 0), *r),
        [(thick - 2, north, span)], superheat_excess, liquid_indicator, ylo, yhi,
        scratch=[VMEM((thick, north, span), f32)], name="heat",
    )
    pressure, residual, heated = call(
        lambda *r: spread_body(dims[0], *r), outs, both, inner, name="spread"
    )
    return heated, pressure, residual


def solution(mesh):
    spec = P("wide", "narrow", None)
    return jax.shard_map(
        on_device,
        mesh=mesh,
        in_specs=(spec, spec, spec, P(), P()),
        out_specs=(spec, spec, spec),
        check_vma=False,
    )
```

```python
import math

import jax
import jax.numpy as jnp
import numpy as np
from jax import lax
from jax.experimental import pallas as pl
from jax.experimental.pallas import tpu as pltpu
from jax.sharding import PartitionSpec as P


ITERS = 3

conduct_liquid = 1.0
conduct_vapor = 0.4
diffusion = 0.06
mobility_liquid = 1.0
mobility_vapor = 4.0
expansion = 0.3
compress = 0.01
highest = lax.Precision.HIGHEST
f32 = jnp.float32
LANES = 128
VMEM = pltpu.VMEM
ORDER = ("narrow", "wide")


def mat(a, b):
    return lax.dot_general(
        a, b, (((1,), (0,)), ((), ())), precision=highest, preferred_element_type=f32
    )


def mat_t(a, b):
    return lax.dot_general(
        a, b, (((1,), (1,)), ((), ())), precision=highest, preferred_element_type=f32
    )


def cosine(m):
    k = np.arange(m)[:, None]
    i = np.arange(m)[None, :]
    scale = np.where(k == 0, math.sqrt(1.0 / m), math.sqrt(2.0 / m))
    return scale * np.cos(np.pi * (k * (2 * i + 1) % (4 * m)) / (2 * m))


def eigen(m):
    return 4.0 * np.sin(np.pi * np.arange(m) / (2 * m)) ** 2


def tables(depth, rows, span, blocks):
    half = depth // 2
    c_z, c_r, c_x = cosine(depth), cosine(rows), cosine(span)
    order = np.concatenate([np.arange(0, depth, 2), np.arange(1, depth, 2)])
    forward = []
    for parity in range(2):
        c = c_z[parity::2, :half]
        forward.append(
            np.einsum("ky,mz->kmzy", c_r, c).reshape(rows * half, half * rows)
        )
    c_sorted = c_z[order]
    swap = np.zeros((2 * depth, 2 * depth))
    swap[:depth, :depth] = c_sorted.T
    swap[depth:, depth:] = c_sorted.T
    shift = eigen(depth)[order][:, None] + eigen(span)[None, :] + compress
    lam = eigen(rows)
    first, last = c_r[:, 0], c_r[:, rows - 1]
    den = lam[None, :, None] + shift[:, None, :]
    same = ((first**2)[None, :, None] / den).sum(1)
    cross = ((first * last)[None, :, None] / den).sum(1)
    m = np.arange(1, blocks)
    sine = np.zeros((blocks, blocks))
    sine[: blocks - 1, : blocks - 1] = math.sqrt(2.0 / blocks) * np.sin(
        np.pi * m[:, None] * m[None, :] / blocks
    )
    wave = np.zeros((blocks, 1))
    wave[: blocks - 1, 0] = 2.0 * np.cos(np.pi * m / blocks)
    return {
        "c_x": c_x.astype(np.float32),
        "forward": np.stack(forward).astype(np.float32),
        "inverse": np.stack([f.T for f in forward]).astype(np.float32),
        "swap": swap.astype(np.float32),
        "shift": shift.astype(np.float32),
        "lam": [float(v) for v in lam],
        "first": [float(v) for v in first],
        "last": [float(v) for v in last],
        "pair": np.stack([1.0 + 2.0 * same, cross], 1).astype(np.float32),
        "sine": sine.astype(np.float32),
        "wave": np.broadcast_to(wave, (blocks, LANES)).astype(np.float32).copy(),
    }


def call(body, outs, *args, smem=(), far=(), far_out=False, scratch=(), flops=1e9):
    specs = [
        pl.BlockSpec(memory_space=pltpu.SMEM if i in smem else pl.ANY if i in far else VMEM)
        for i in range(len(args))
    ]
    return pl.pallas_call(
        body,
        out_shape=[jax.ShapeDtypeStruct(s, f32) for s in outs],
        in_specs=specs,
        out_specs=[pl.BlockSpec(memory_space=pl.ANY if far_out else VMEM)] * len(outs),
        scratch_shapes=list(scratch),
        compiler_params=pltpu.CompilerParams(vmem_limit_bytes=16 * 2**20),
        cost_estimate=pl.CostEstimate(flops=int(flops), bytes_accessed=4 << 20, transcendentals=0),
    )(*args)


def row_roll(x, up):
    n = x.shape[0]
    if n % 8 == 0:
        return pltpu.roll(x, n - 1 if up else 1, 0)
    if up:
        return jnp.concatenate([x[1:], x[:1]], 0)
    return jnp.concatenate([x[-1:], x[:-1]], 0)


def lane_roll(x, up):
    n = x.shape[1]
    return pltpu.roll(x, n - 1 if up else 1, 1)


def fold_lanes(x):
    total = x[:, :LANES]
    for i in range(1, x.shape[1] // LANES):
        total = total + x[:, i * LANES : (i + 1) * LANES]
    return jnp.sum(total, axis=0, keepdims=True)


def smear_blocks(smear, size):
    n = smear.shape[0]
    i = lax.broadcasted_iota(jnp.int32, (n, size), 0)
    j = lax.broadcasted_iota(jnp.int32, (n, size), 1)
    wide_pick = jnp.where(i == j % n, 1.0, 0.0)
    i = lax.broadcasted_iota(jnp.int32, (size, n), 0)
    j = lax.broadcasted_iota(jnp.int32, (size, n), 1)
    tall_pick = jnp.where(i % n == j, 1.0, 0.0)
    tiled = mat(tall_pick, mat(smear, wide_pick))
    i = lax.broadcasted_iota(jnp.int32, (size, size), 0)
    j = lax.broadcasted_iota(jnp.int32, (size, size), 1)
    return jnp.where(i // n == j // n, tiled, 0.0)


def conducted(t, p, pairs):
    flux = jnp.zeros_like(t)
    faces = jnp.zeros_like(t)
    for near_t, near_p in pairs:
        differ = near_p != p
        flux = flux + jnp.where(differ, -2.0 * t, near_t - t)
        faces = faces + jnp.where(differ, 1.0, 0.0)
    k = jnp.where(p > 0.5, conduct_liquid, conduct_vapor)
    value = t + diffusion * k * flux
    return value, 2.0 * k * faces * value


def heat_body(dims, inner, *refs):
    thick, north, span, size_y, size_x, most = dims
    if inner:
        (table, temp, phase, ylo, yhi, smear, smear_e, heated, source, mob, pp, mass, mask) = refs
        tp = temp
    else:
        (table, temp, phase, zlo, zhi, ylo, yhi, smear, smear_e,
         heated, source, tp, pp, mass, mask) = refs
    skip = 1 if inner else 0
    base = 1 - skip
    planes = thick - 2 * skip
    tiles_y = north // size_y
    tiles_x = span // size_x
    w, n = lax.axis_index("wide"), lax.axis_index("narrow")
    n_first, n_last = n == 0, n == lax.axis_size("narrow") - 1
    for z in range(thick):
        pp[z + base] = phase[z].astype(f32)
        if inner:
            mob[z] = jnp.where(pp[z] > 0.5, mobility_liquid, mobility_vapor)
        else:
            tp[z + 1] = temp[z]
    if not inner:
        w_first, w_last = w == 0, w == lax.axis_size("wide") - 1
        tp[0] = jnp.where(w_first, temp[0], zlo[0])
        pp[0] = jnp.where(w_first, phase[0].astype(f32), zlo[1])
        tp[thick + 1] = jnp.where(w_last, temp[thick - 1], zhi[0])
        pp[thick + 1] = jnp.where(w_last, phase[thick - 1].astype(f32), zhi[1])
    row = lax.broadcasted_iota(jnp.int32, (tiles_y, span), 0)
    lane = lax.broadcasted_iota(jnp.int32, (tiles_y, span), 1)
    tile = row * tiles_x + lane // size_x
    hit = tile == table[0]
    for i in range(1, most):
        hit = jnp.logical_or(hit, tile == table[i])
    mask[...] = jnp.where(hit, expansion, 0.0)
    r = lax.broadcasted_iota(jnp.int32, (size_y, span), 0)
    c = lax.broadcasted_iota(jnp.int32, (size_y, span), 1)

    def plane(z):
        for yc in range(tiles_y):
            at = pl.ds(yc * size_y, size_y)
            t = tp[z + base, at, :]
            p = pp[z + base, at, :]

            def edge(ref, halo, k, y, wall, own):
                if 0 <= y < north:
                    return ref[z + base, pl.ds(y, 1), :]
                return jnp.where(wall, own, halo[k, z])

            pairs = [
                (tp[z + base - 1, at, :], pp[z + base - 1, at, :]),
                (tp[z + base + 1, at, :], pp[z + base + 1, at, :]),
                (jnp.where(c == span - 1, t, lane_roll(t, True)),
                 jnp.where(c == span - 1, p, lane_roll(p, True))),
                (jnp.where(c == 0, t, lane_roll(t, False)),
                 jnp.where(c == 0, p, lane_roll(p, False))),
            ]
            y = (yc + 1) * size_y
            pairs.append((
                jnp.where(r == size_y - 1, edge(tp, yhi, 0, y, n_last, t[size_y - 1:]), row_roll(t, True)),
                jnp.where(r == size_y - 1, edge(pp, yhi, 1, y, n_last, p[size_y - 1:]), row_roll(p, True)),
            ))
            y = yc * size_y - 1
            pairs.append((
                jnp.where(r == 0, edge(tp, ylo, 0, y, n_first, t[:1]), row_roll(t, False)),
                jnp.where(r == 0, edge(pp, ylo, 1, y, n_first, p[:1]), row_roll(p, False)),
            ))
            value, vapor = conducted(t, p, pairs)
            heated[z - skip, at, :] = value
            to = pl.ds(pl.multiple_of((z - skip) * north, north) + yc * size_y, size_y)
            mass[to, :] = vapor

    lax.fori_loop(skip, thick - skip, lambda z, carry: (plane(z), carry)[1], 0)
    smear_n = smear_blocks(smear[...], north)
    for tx in range(tiles_x):
        at = slice(tx * size_x, (tx + 1) * size_x)
        mass[:, at] = mat_t(mass[:, at], smear_e[...])
    for z in range(planes):
        smeared = mat(smear_n, mass[z * north : (z + 1) * north, :])
        for yc in range(tiles_y):
            part = smeared[yc * size_y : (yc + 1) * size_y] * mask[yc : yc + 1, :]
            if inner:
                source[z, yc * size_y : (yc + 1) * size_y, :] = part
            else:
                source[yc, z] = part


def pack_body(dims, listing, far_temp, far_phase, out, side_first, side_last, temp, phase, entry, sems):
    wide, thick, rows, span, most = dims
    tiles = span // LANES
    per = thick * tiles * rows
    north = wide * rows
    copies = [
        pltpu.make_async_copy(far_temp, temp, sems.at[0]),
        pltpu.make_async_copy(far_phase, phase, sems.at[1]),
    ]
    for copy in copies:
        copy.start()
    entry[...] = jnp.full((8, LANES), -1.0, f32)
    entry[0:1, 0:most] = listing[0].astype(f32)
    odd = lax.axis_index("narrow") % 2 == 1
    for w in range(wide):
        out[w, 2 * per :, :] = entry[...]
    for a, ref in enumerate((temp, phase)):
        copies[a].wait()
        for z in range(thick):
            side_first[a, z] = ref[z, 0:1, :].astype(f32)
            side_last[a, z] = ref[z, north - 1 : north, :].astype(f32)
            for w in range(wide):
                for t in range(tiles):
                    at = a * per + (z * tiles + t) * rows
                    piece = ref[z, w * rows : (w + 1) * rows, t * LANES : (t + 1) * LANES]
                    out[jnp.where(odd, wide - 1 - w, w), at : at + rows, :] = piece.astype(f32)


def edge_body(dims, got, first, last):
    wide, thick, rows, span, _ = dims
    tiles = span // LANES
    per = thick * tiles * rows
    for a in range(2):
        for w in range(wide):
            for z in range(thick):
                for t in range(tiles):
                    at = a * per + (z * tiles + t) * rows
                    row = a * wide * thick + w * thick + z
                    lanes = slice(t * LANES, (t + 1) * LANES)
                    first[row : row + 1, lanes] = got[w, at : at + 1, :]
                    last[row : row + 1, lanes] = got[w, at + rows - 1 : at + rows, :]


def boil_body(dims, tab, got, lo, hi, smear, smear_e, fwd, c_x, shift,
              source, mob, mob_lo, mob_hi, spec, message, outer, tp, pp, mass, heated, mask, entries):
    wide, thick, rows, span, _ = dims
    depth = wide * thick
    tiles = span // LANES
    per = thick * tiles * rows
    size_x = smear_e.shape[0]
    w, n = lax.axis_index("wide"), lax.axis_index("narrow")
    chunk = jnp.where(n % 2 == 1, wide - 1 - w, w)
    own = n * wide + chunk
    for w in range(wide):
        entries[w : w + 1, :] = got[w, 2 * per : 2 * per + 1, :]
        for z in range(thick):
            for t in range(tiles):
                at = (z * tiles + t) * rows
                to = ((w * thick + z) * rows, t * LANES)
                to = (slice(to[0], to[0] + rows), slice(to[1], to[1] + LANES))
                tp[to] = got[w, at : at + rows, :]
                pp[to] = got[w, per + at : per + at + rows, :]
    for tx in range(span // size_x):
        tile = (chunk * (span // size_x) + tx).astype(f32)
        hit = jnp.where(entries[...] == tile, expansion, 0.0)
        hit = jnp.max(hit, axis=1, keepdims=True)
        mask[:, tx * size_x : (tx + 1) * size_x] = jnp.broadcast_to(hit, (wide, size_x))
    mob[...] = jnp.where(pp[...] > 0.5, mobility_liquid, mobility_vapor)
    mob_lo[...] = jnp.where(lo[depth:, :] > 0.5, mobility_liquid, mobility_vapor)
    mob_hi[...] = jnp.where(hi[depth:, :] > 0.5, mobility_liquid, mobility_vapor)
    r = lax.broadcasted_iota(jnp.int32, (rows, span), 0)
    c = lax.broadcasted_iota(jnp.int32, (rows, span), 1)
    no_lo, no_hi = own == 0, own == lax.axis_size("narrow") * wide - 1

    def at_z(z):
        return pl.ds(pl.multiple_of(z * rows, rows), rows)

    def slab(z):
        t, p = tp[at_z(z), :], pp[at_z(z), :]
        below, above = at_z(jnp.maximum(z - 1, 0)), at_z(jnp.minimum(z + 1, depth - 1))

        def along_y(x, k, up):
            if up:
                edge = jnp.where(no_hi, x[rows - 1 :], hi[pl.ds(k * depth + z, 1), :])
                return jnp.where(r == rows - 1, edge, row_roll(x, True))
            edge = jnp.where(no_lo, x[:1], lo[pl.ds(k * depth + z, 1), :])
            return jnp.where(r == 0, edge, row_roll(x, False))

        pairs = [
            (tp[below, :], pp[below, :]),
            (tp[above, :], pp[above, :]),
            (along_y(t, 0, True), along_y(p, 1, True)),
            (along_y(t, 0, False), along_y(p, 1, False)),
            (jnp.where(c == span - 1, t, lane_roll(t, True)),
             jnp.where(c == span - 1, p, lane_roll(p, True))),
            (jnp.where(c == 0, t, lane_roll(t, False)),
             jnp.where(c == 0, p, lane_roll(p, False))),
        ]
        heated[at_z(z), :], mass[at_z(z), :] = conducted(t, p, pairs)

    lax.fori_loop(0, depth, lambda z, carry: (slab(z), carry)[1], 0)
    for w in range(wide):
        for k, z in enumerate((w * thick, (w + 1) * thick - 1)):
            outer[w, k * rows : (k + 1) * rows, :] = heated[z * rows : (z + 1) * rows, :]
    for tx in range(span // size_x):
        at = slice(tx * size_x, (tx + 1) * size_x)
        mass[:, at] = mat_t(mass[:, at], smear_e[...])
    group = LANES
    smear_n = smear_blocks(smear[...], group)
    for g in range(depth * rows // group):
        smeared = mat(smear_n, mass[g * group : (g + 1) * group, :])
        for i in range(group // rows):
            z = g * (group // rows) + i
            source[z * rows : (z + 1) * rows, :] = (
                smeared[i * rows : (i + 1) * rows] * mask[z // thick : z // thick + 1, :]
            )
    forward_body(
        (depth, rows, span), tab, source, mass, spec, fwd, c_x, shift, message,
        jnp.zeros((1, LANES), f32),
    )


def finish_body(dims, rho, parts, p, r, d, image, *refs):
    outer, out = refs if len(refs) == 2 else (None, refs[0])
    wide, thick, rows, span, _ = dims
    total = parts[0]
    for i in range(1, parts.shape[0]):
        total = total + parts[i]
    alpha = (rho[...] / jnp.sum(total, axis=1, keepdims=True))[:, :1]
    n = thick * rows
    tiles = span // LANES
    for w in range(wide):
        at = slice(w * n, (w + 1) * n)
        pressure = p[at, :] + alpha * d[at, :]
        residual = r[at, :] - alpha * image[at, :]
        if outer is None:
            out[w, :n, :] = pressure
            out[w, n : 2 * n, :] = residual
            continue
        units = [pressure[z * rows : (z + 1) * rows] for z in range(thick)]
        units += [residual[z * rows : (z + 1) * rows] for z in (0, thick - 1)]
        units += [outer[w, :rows, :], outer[w, rows:, :]]
        for u, unit in enumerate(units):
            for t in range(tiles):
                to = (u * tiles + t) * rows
                out[w, to : to + rows, :] = unit[:, t * LANES : (t + 1) * LANES]
        to = len(units) * tiles * rows
        for z in range(1, thick - 1):
            for y in (z * rows, (z + 1) * rows - 1):
                for t in range(tiles):
                    out[w, to : to + 1, :] = residual[y : y + 1, t * LANES : (t + 1) * LANES]
                    to += 1


def spread_body(dims, got, pressure, residual):
    wide, thick, rows, _, _ = dims
    for k, out in enumerate((pressure, residual)):
        for z in range(thick):
            row = (k * thick + z) * rows
            for w in range(wide):
                out[z, w * rows : (w + 1) * rows, :] = got[w, row : row + rows, :]


def gather_body(dims, got, inner, source, mob, *refs):
    wide, thick, rows, span, _ = dims
    tiles = span // LANES
    north = wide * rows
    pressure, residual, heated = refs[3:6]
    copies = [pltpu.make_async_copy(refs[3 + i], refs[i], refs[6].at[i]) for i in range(3)]
    odd = lax.axis_index("narrow") % 2 == 1
    planes = [(pressure, z) for z in range(thick)]
    planes += [(out, z) for out in (residual, heated) for z in (0, thick - 1)]
    for w in range(wide):
        chunk = jnp.where(odd, wide - 1 - w, w)
        y = pl.ds(pl.multiple_of(chunk * rows, rows), rows)
        for u, (out, z) in enumerate(planes):
            for t in range(tiles):
                at = (u * tiles + t) * rows
                out[z, y, t * LANES : (t + 1) * LANES] = got[w, at : at + rows, :]
    for z in range(1, thick - 1):
        heated[z] = inner[z - 1]
    copies[0].start()
    copies[2].start()
    r = lax.broadcasted_iota(jnp.int32, (rows, span), 0)
    c = lax.broadcasted_iota(jnp.int32, (rows, span), 1)
    for z in range(1, thick - 1):

        def part(i, z=z):
            start = pl.multiple_of(i * rows, rows)
            at = pl.ds(start, rows)
            v, b = pressure[z, at, :], mob[z, at, :]
            flux = jnp.where(c == span - 1, 0.0, (b + lane_roll(b, True)) * (v - lane_roll(v, True)))
            total = flux - lane_roll(flux, False)
            for k in (z - 1, z + 1):
                total = total + (b + mob[k, at, :]) * (v - pressure[k, at, :])
            y = jnp.minimum(start + rows, north - 1)
            v_hi = jnp.where(r == rows - 1, pressure[z, pl.ds(y, 1), :], row_roll(v, True))
            b_hi = jnp.where(r == rows - 1, mob[z, pl.ds(y, 1), :], row_roll(b, True))
            y = jnp.maximum(start - 1, 0)
            v_lo = jnp.where(r == 0, pressure[z, pl.ds(y, 1), :], row_roll(v, False))
            b_lo = jnp.where(r == 0, mob[z, pl.ds(y, 1), :], row_roll(b, False))
            total = total + (b + b_hi) * (v - v_hi) + (b + b_lo) * (v - v_lo)
            residual[z, at, :] = source[z - 1, at, :] - (compress * v + 0.5 * total)

        lax.fori_loop(0, wide, lambda i, carry: (part(i), carry)[1], 0)
        first = len(planes) * tiles * rows + (z - 1) * 2 * tiles
        for side, y in enumerate((0, north - 1)):
            lower = 0 if side == 0 else wide - 1
            w = jnp.where(odd, wide - 1 - lower, lower)
            for t in range(tiles):
                at = first + side * tiles + t
                residual[z, y : y + 1, t * LANES : (t + 1) * LANES] = got[w, at : at + 1, :]
    copies[1].start()
    for copy in copies:
        copy.wait()


def forward_body(dims, tab, field, fold, spec, fwd, c_x, shift, message, extra):
    depth, rows, span = dims
    half = depth // 2
    size = half * rows
    for parity in range(2):
        for z in range(half):
            a = field[z * rows : (z + 1) * rows, :]
            b = field[(depth - 1 - z) * rows : (depth - z) * rows, :]
            fold[z * rows : (z + 1) * rows, :] = a + b if parity == 0 else a - b
        spec[parity * size : (parity + 1) * size, :] = mat_t(
            mat(fwd[parity], fold[:size, :]), c_x[...]
        )
    for parity in range(2):
        mu = shift[parity * half : (parity + 1) * half, :]
        low = jnp.zeros((half, span), f32)
        high = jnp.zeros((half, span), f32)
        for ky in range(rows):
            at = parity * size + ky * half
            g = spec[at : at + half, :] / (mu + tab["lam"][ky])
            low = low + tab["first"][ky] * g
            high = high + tab["last"][ky] * g
        for k in range(half):
            o = parity * half + k
            message[o, 0:1, :span] = low[k : k + 1]
            message[o, 0:1, span : 2 * span] = high[k : k + 1]
            message[o, 0:1, 2 * span :] = extra


def start_body(dims, tab, source, fwd, c_x, shift, spec, message, fold):
    forward_body(dims, tab, source, fold, spec, fwd, c_x, shift, message, jnp.zeros((1, LANES), f32))


def solve_body(dims, tab, first_call, seats, *refs):
    depth, rows, span = dims
    half = depth // 2
    if first_call:
        (got, spec, shift, pairs, sine, wave, h_new, message, low, high) = refs
    else:
        (got, spec, shift, pairs, sine, wave, image_spec, h_old, rho,
         spec_new, h_new, message, alpha_out, low, high) = refs
    pair = pairs[lax.axis_index("narrow") * lax.axis_size("wide") + lax.axis_index("wide")]
    blocks = len(seats)
    for j, i in enumerate(seats):
        low[j : j + 1, :] = got[i, 0:1, :span]
        high[j : j + 1, :] = got[i, 0:1, span : 2 * span]
    jump = high[...] - row_roll(low[...], True)
    r = lax.broadcasted_iota(jnp.int32, (blocks, span), 0)
    jump = jnp.where(r == blocks - 1, 0.0, jump)
    if not first_call:
        bottom = jnp.zeros((1, LANES), f32)
        for j in range(blocks):
            bottom = bottom + got[j, 0:1, 2 * span :]
        alpha = rho[...] / jnp.sum(bottom, axis=1, keepdims=True)
        alpha_out[...] = alpha
        alpha = alpha[:, :1]
        jump = h_old[...] - alpha * jump
    h_new[...] = jump
    scale = 1.0 / (pair[0:1, :] - wave[:, :1] * pair[1:2, :])
    q = mat(sine[...], mat(sine[...], jump) * scale)
    total = fold_lanes(q * jump) * -1.0
    acc = jnp.zeros((8, span), f32)
    for parity in range(2):
        mu = shift[parity * half : (parity + 1) * half, :]
        for ky in range(rows):
            at = parity * half * rows + ky * half
            s = spec[at : at + half, :]
            if not first_call:
                s = s - alpha * image_spec[at : at + half, :]
                spec_new[at : at + half, :] = s
            e = s * s / (mu + tab["lam"][ky])
            for i in range(half // 8):
                acc = acc + e[i * 8 : (i + 1) * 8]
    total = total + fold_lanes(acc)
    zero = jnp.zeros((1, span), f32)
    for j, i in enumerate(seats):
        message[i, 0:1, :span] = zero if j == 0 else q[j - 1 : j]
        message[i, 0:1, span : 2 * span] = q[j : j + 1]
        message[i, 0:1, 2 * span :] = total


def advance_body(dims, tab, first_call, last_call, blocks, *refs):
    depth, rows, span = dims
    half = depth // 2
    size = half * rows
    refs = list(refs)
    take = refs.pop
    if last_call:
        n = ITERS - 1
        at = 13
        refs[at : at + 3 * n] = [refs[at : at + n], refs[at + n : at + 2 * n], refs[at + 2 * n : at + 3 * n]]
    got, spec, shift, inv, fwd, c_x, swap, mob, mob_lo, mob_hi = [take(0) for _ in range(10)]
    if not first_call:
        dir_old, q_old, rho_old = [take(0) for _ in range(3)]
    if last_call:
        alphas, olds, images, source = take(0), take(0), take(0), take(0)
    direction, image = take(0), take(0)
    if last_call:
        rho_out, part_out, p_out, r_out = [take(0) for _ in range(4)]
    else:
        rho_out, dir_spec, q_out, image_spec, message = [take(0) for _ in range(5)]
    work, q_mid, fold = take(0), take(0), take(0)
    if last_call:
        dir_spec, q_out = take(0), take(0)

    total = jnp.zeros((1, LANES), f32)
    for o in range(depth):
        q_mid[o : o + 1, :] = got[o, 0:1, :span]
        q_mid[depth + o : depth + o + 1, :] = got[o, 0:1, span : 2 * span]
        total = total + got[o, 0:1, 2 * span :]
    rho = jnp.sum(total, axis=1, keepdims=True) + jnp.zeros((1, LANES), f32)
    rho_out[...] = rho
    if not first_call:
        beta = (rho / rho_old[...])[:, :1]
    for parity in range(2):
        at_q = parity * half
        mu = shift[at_q : at_q + half, :]
        q_lo = q_mid[at_q : at_q + half, :]
        q_hi = q_mid[depth + at_q : depth + at_q + half, :]
        for ky in range(rows):
            at = parity * size + ky * half
            u = (spec[at : at + half, :] + tab["first"][ky] * q_lo - tab["last"][ky] * q_hi) / (
                mu + tab["lam"][ky]
            )
            if not first_call:
                u = u + beta * dir_old[at : at + half, :]
            dir_spec[at : at + half, :] = u
    q = q_mid[...]
    if not first_call:
        q = q + beta * q_old[...]
    q_out[...] = q
    q_mid[...] = mat(swap[...], mat(q, c_x[...]))
    for parity in range(2):
        fold[parity * size : (parity + 1) * size, :] = mat(
            inv[parity], mat(dir_spec[parity * size : (parity + 1) * size, :], c_x[...])
        )
    for z in range(half):
        a = fold[z * rows : (z + 1) * rows, :]
        b = fold[size + z * rows : size + (z + 1) * rows, :]
        direction[z * rows : (z + 1) * rows, :] = a + b
        direction[(depth - 1 - z) * rows : (depth - z) * rows, :] = a - b

    r = lax.broadcasted_iota(jnp.int32, (rows, span), 0)
    c = lax.broadcasted_iota(jnp.int32, (rows, span), 1)
    acc = jnp.zeros((1, span), f32)
    below = None
    for z in range(depth):
        at = slice(z * rows, (z + 1) * rows)
        v = direction[at, :]
        b = mob[at, :]
        out = compress * v
        flux = jnp.where(c == span - 1, 0.0, (b + lane_roll(b, True)) * (v - lane_roll(v, True)))
        out_flux = flux - lane_roll(flux, False)
        b_hi = b[rows - 1 :] + mob_hi[z : z + 1, :]
        flux = jnp.where(
            r == rows - 1,
            b_hi * q_mid[depth + z : depth + z + 1, :],
            (b + row_roll(b, True)) * (v - row_roll(v, True)),
        )
        f_lo = (b[:1] + mob_lo[z : z + 1, :]) * q_mid[z : z + 1, :]
        out_flux = out_flux + flux - jnp.where(r == 0, f_lo, row_roll(flux, False))
        if below is not None:
            out_flux = out_flux - below
        if z + 1 < depth:
            up = slice((z + 1) * rows, (z + 2) * rows)
            below = (b + mob[up, :]) * (v - direction[up, :])
            out_flux = out_flux + below
        out = out + 0.5 * out_flux
        image[at, :] = out
        acc = acc + jnp.sum(v * out, axis=0, keepdims=True)
    part = fold_lanes(acc)
    if last_call:
        for i in range(blocks):
            part_out[i] = part
        p = alphas[0][:, :1] * olds[0][...]
        r = source[...] - alphas[0][:, :1] * images[0][...]
        for i in range(1, len(olds)):
            p = p + alphas[i][:, :1] * olds[i][...]
            r = r - alphas[i][:, :1] * images[i][...]
        p_out[...] = p
        r_out[...] = r
    else:
        forward_body(dims, tab, image, work, image_spec, fwd, c_x, shift, message, part)


def split_by_z(superheat_excess, liquid_indicator, listing, smear_n, smear_e, dims, const):
    thick, north, span = superheat_excess.shape
    wide, lanes = lax.axis_size("wide"), lax.axis_size("narrow")
    depth, rows, span = dims[1]
    size_y, size_x = smear_n.shape[0], smear_e.shape[0]
    tiles_y = north // size_y
    whole = depth * rows
    phase = liquid_indicator.astype(f32)
    both = jnp.stack([superheat_excess, phase])
    up = [(i, i + 1) for i in range(wide - 1)]
    down = [(i + 1, i) for i in range(wide - 1)]
    zlo = lax.ppermute(both[:, thick - 1], "wide", up)
    zhi = lax.ppermute(both[:, 0], "wide", down)
    up = [(i, i + 1) for i in range(lanes - 1)]
    down = [(i + 1, i) for i in range(lanes - 1)]
    ylo = lax.ppermute(both[:, :, north - 1 :], "narrow", up)
    yhi = lax.ppermute(both[:, :, :1], "narrow", down)

    def regroup(x):
        x = x.reshape(wide, thick * rows, span)
        return lax.all_to_all(x, "wide", split_axis=0, concat_axis=0, tiled=True)

    mob = jnp.where(phase > 0.5, mobility_liquid, mobility_vapor)
    mob = mob.reshape(thick, wide, rows, span).transpose(1, 0, 2, 3)
    mob = regroup(mob).reshape(depth, rows, span)
    most = listing.size
    heat_dims = (thick, north, span, size_y, size_x, most)
    heated, source = call(
        lambda *r: heat_body(heat_dims, False, *r),
        [(thick, north, span), (tiles_y, thick, size_y, span)],
        listing.reshape(-1), superheat_excess, liquid_indicator, zlo, zhi, ylo, yhi,
        smear_n, smear_e,
        smem=(0,),
        scratch=[
            VMEM((thick + 2, north, span), f32),
            VMEM((thick + 2, north, span), f32),
            VMEM((thick * north, span), f32),
            VMEM((tiles_y, span), f32),
        ],
    )
    source, mob = lax.optimization_barrier((source, mob))
    if size_y != rows:
        source = source.transpose(1, 0, 2, 3).reshape(thick, wide, rows, span).transpose(1, 0, 2, 3)
    source = regroup(source).reshape(whole, span)
    up, down = const["row_pairs"]
    mob_lo = lax.ppermute(mob[:, rows - 1], ("wide", "narrow"), up)
    mob_hi = lax.ppermute(mob[:, 0], ("wide", "narrow"), down)
    spec, message = call(
        lambda *r: start_body(dims[1], const["tab"], *r), [(whole, span), const["letter"]],
        source, const["forward"], const["c_x"], const["shift"],
        scratch=[VMEM((whole, span), f32)],
    )
    return heated, source, mob.reshape(whole, span), mob_lo, mob_hi, spec, message


def split_by_y(superheat_excess, liquid_indicator, listing, smear_n, smear_e, dims, const):
    depth, rows, span = dims[1]
    wide, thick = dims[0][:2]
    lanes = lax.axis_size("narrow")
    whole = depth * rows
    per = thick * rows * (span // LANES)
    north = superheat_excess.shape[1]
    packed, side_first, side_last = call(
        lambda *r: pack_body(dims[0], *r),
        [(wide, 2 * per + 8, LANES), (2, thick, 1, span), (2, thick, 1, span)],
        listing, superheat_excess, liquid_indicator, far=(1, 2),
        scratch=[
            VMEM((thick, north, span), f32),
            VMEM((thick, north, span), jnp.int32),
            VMEM((8, LANES), f32),
            pltpu.SemaphoreType.DMA((2,)),
        ],
    )
    got = lax.all_to_all(packed, "wide", split_axis=0, concat_axis=0, tiled=True)
    first, last = call(lambda *r: edge_body(dims[0], *r), [(2 * depth, span)] * 2, got)
    up, down = const["row_pairs"]
    lo = lax.ppermute(last, ("wide", "narrow"), up)
    hi = lax.ppermute(first, ("wide", "narrow"), down)
    full, plane = (whole, span), (depth, span)
    y_up = [(i, i + 1) for i in range(lanes - 1)]
    y_down = [(i + 1, i) for i in range(lanes - 1)]
    ylo = lax.ppermute(side_last, "narrow", y_up)
    yhi = lax.ppermute(side_first, "narrow", y_down)
    block, inner = (thick, north, span), (thick - 2, north, span)
    size_y, size_x = smear_n.shape[0], smear_e.shape[0]
    heat_dims = (thick, north, span, size_y, size_x, listing.size)
    middle = call(
        lambda *r: heat_body(heat_dims, True, *r),
        [inner, inner, block],
        listing.reshape(-1), superheat_excess, liquid_indicator, ylo, yhi, smear_n, smear_e,
        smem=(0,),
        scratch=[
            VMEM(block, f32),
            VMEM(((thick - 2) * north, span), f32),
            VMEM((north // size_y, span), f32),
        ],
    )
    lo, hi, *middle = lax.optimization_barrier((lo, hi, *middle))
    return middle, *call(
        lambda *r: boil_body(dims[0], const["tab"], *r),
        [full, full, plane, plane, full, const["letter"], (wide, 2 * rows, span)],
        got, lo, hi, smear_n, smear_e, const["forward"], const["c_x"], const["shift"],
        scratch=[VMEM(full, f32)] * 4 + [VMEM((wide, span), f32), VMEM((wide, LANES), f32)],
    )


def on_device(superheat_excess, liquid_indicator, listing, smear_n, smear_e):
    thick, north, span = superheat_excess.shape
    wide, lanes = lax.axis_size("wide"), lax.axis_size("narrow")
    blocks = wide * lanes
    depth = thick * wide
    rows = north // wide
    size_y = smear_n.shape[0]
    shape = (depth, rows, span)
    dims = ((wide, thick, rows, span, listing.size), shape)
    tab = tables(depth, rows, span, blocks)
    whole = depth * rows
    full, one = (whole, span), (1, LANES)
    letter = (blocks, 1, 2 * span + LANES)

    by_y = rows == size_y and thick > 2

    def seat(j):
        n, c = j // wide, j % wide
        return n, wide - 1 - c if by_y and n % 2 == 1 else c

    def place(j):
        n, w = seat(j)
        return w * lanes + n

    seats = [n * wide + w for n, w in map(seat, range(blocks))]
    up = [(place(j), place(j + 1)) for j in range(blocks - 1)]
    const = {k: jnp.asarray(tab[k]) for k in ("c_x", "forward", "inverse", "swap", "shift", "pair", "sine", "wave")}
    const["tab"], const["letter"] = tab, letter
    const["row_pairs"] = up, [(b, a) for a, b in up]
    if by_y:
        middle, source, mob, mob_lo, mob_hi, spec, message, outer = split_by_y(
            superheat_excess, liquid_indicator, listing, smear_n, smear_e, dims, const
        )
    else:
        heated, source, mob, mob_lo, mob_hi, spec, message = split_by_z(
            superheat_excess, liquid_indicator, listing, smear_n, smear_e, dims, const
        )

    def swap_all(x):
        return lax.all_to_all(x, ORDER, split_axis=0, concat_axis=0, tiled=True)

    shift, pair, sine, wave = (const[k] for k in ("shift", "pair", "sine", "wave"))
    pair_scratch = [VMEM((blocks, span), f32)] * 2
    jump, message = call(
        lambda *r: solve_body(shape, tab, True, seats, *r), [(blocks, span), letter],
        swap_all(message), spec, shift, pair, sine, wave, scratch=pair_scratch,
    )
    dir_spec = q = rho = None
    directions, images, alphas = [], [], []
    for iteration in range(ITERS):
        first, final = iteration == 0, iteration + 1 == ITERS
        args = [swap_all(message), spec, shift, const["inverse"], const["forward"], const["c_x"], const["swap"], mob, mob_lo, mob_hi]
        if not first:
            args += [dir_spec, q, rho]
        outs = [full, full, one]
        work = [VMEM(full, f32), VMEM((2 * depth, span), f32), VMEM(full, f32)]
        if final:
            outs += [(blocks, 1, LANES), full, full]
            args += [*alphas, *directions, *images, source]
            work += [VMEM(full, f32), VMEM((2 * depth, span), f32)]
        else:
            outs += [full, (2 * depth, span), full, letter]
        result = call(
            lambda *r, a=first, b=final: advance_body(shape, tab, a, b, blocks, *r), outs, *args,
            scratch=work,
        )
        directions.append(result[0])
        images.append(result[1])
        rho = result[2]
        if final:
            parts = swap_all(result[3])
            pressure, residual = result[4:]
        else:
            dir_spec, q, image_spec, message = result[3:]
            spec, jump, message, alpha = call(
                lambda *r: solve_body(shape, tab, False, seats, *r),
                [full, (blocks, span), letter, one],
                swap_all(message), spec, shift, pair, sine, wave, image_spec, jump, rho,
                scratch=pair_scratch,
            )
            alphas.append(alpha)

    if by_y:
        extra = [outer]
        tiles = span // LANES
        lines = (thick + 4) * rows * tiles + -(-2 * (thick - 2) * tiles // 8) * 8
        packet = (wide, lines, LANES)
    else:
        extra = []
        packet = (wide, 2 * thick * rows, span)
    (both,) = call(
        lambda *r: finish_body(dims[0], *r), [packet],
        rho, parts, pressure, residual, directions[2], images[2], *extra,
    )
    both = lax.all_to_all(both, "wide", split_axis=0, concat_axis=0, tiled=True)
    block = (thick, north, span)
    if not by_y:
        pressure, residual = call(lambda *r: spread_body(dims[0], *r), [block] * 2, both)
        return heated, pressure, residual
    pressure, residual, heated = call(
        lambda *r: gather_body(dims[0], *r), [block] * 3, both, *middle, far_out=True,
        scratch=[VMEM(block, f32)] * 3 + [pltpu.SemaphoreType.DMA((3,))],
    )
    return heated, pressure, residual


def solution(mesh):
    spec = P("wide", "narrow", None)
    return jax.shard_map(
        on_device,
        mesh=mesh,
        in_specs=(spec, spec, spec, P(), P()),
        out_specs=(spec, spec, spec),
        check_vma=False,
    )
```

```python
import math

import jax
import jax.numpy as jnp
import numpy as np
from jax import lax
from jax.experimental import pallas as pl
from jax.experimental.pallas import tpu as pltpu
from jax.sharding import PartitionSpec as P


ITERS = 3

conduct_liquid = 1.0
conduct_vapor = 0.4
diffusion = 0.06
mobility_liquid = 1.0
mobility_vapor = 4.0
expansion = 0.3
compress = 0.01
highest = lax.Precision.HIGHEST
f32 = jnp.float32
LANES = 128
VMEM = pltpu.VMEM
ORDER = ("narrow", "wide")


def mat(a, b):
    return lax.dot_general(
        a, b, (((1,), (0,)), ((), ())), precision=highest, preferred_element_type=f32
    )


def mat_t(a, b):
    return lax.dot_general(
        a, b, (((1,), (1,)), ((), ())), precision=highest, preferred_element_type=f32
    )


def cosine(m):
    k = np.arange(m)[:, None]
    i = np.arange(m)[None, :]
    scale = np.where(k == 0, math.sqrt(1.0 / m), math.sqrt(2.0 / m))
    return scale * np.cos(np.pi * (k * (2 * i + 1) % (4 * m)) / (2 * m))


def eigen(m):
    return 4.0 * np.sin(np.pi * np.arange(m) / (2 * m)) ** 2


def tables(depth, rows, span, blocks):
    half = depth // 2
    c_z, c_r, c_x = cosine(depth), cosine(rows), cosine(span)
    order = np.concatenate([np.arange(0, depth, 2), np.arange(1, depth, 2)])
    forward = []
    for parity in range(2):
        c = c_z[parity::2, :half]
        forward.append(
            np.einsum("ky,mz->kmzy", c_r, c).reshape(rows * half, half * rows)
        )
    c_sorted = c_z[order]
    swap = np.zeros((2 * depth, 2 * depth))
    swap[:depth, :depth] = c_sorted.T
    swap[depth:, depth:] = c_sorted.T
    shift = eigen(depth)[order][:, None] + eigen(span)[None, :] + compress
    lam = eigen(rows)
    first, last = c_r[:, 0], c_r[:, rows - 1]
    den = lam[None, :, None] + shift[:, None, :]
    same = ((first**2)[None, :, None] / den).sum(1)
    cross = ((first * last)[None, :, None] / den).sum(1)
    m = np.arange(1, blocks)
    sine = np.zeros((blocks, blocks))
    sine[: blocks - 1, : blocks - 1] = math.sqrt(2.0 / blocks) * np.sin(
        np.pi * m[:, None] * m[None, :] / blocks
    )
    wave = np.zeros((blocks, 1))
    wave[: blocks - 1, 0] = 2.0 * np.cos(np.pi * m / blocks)
    return {
        "c_x": c_x.astype(np.float32),
        "forward": np.stack(forward).astype(np.float32),
        "inverse": np.stack([f.T for f in forward]).astype(np.float32),
        "swap": swap.astype(np.float32),
        "shift": shift.astype(np.float32),
        "lam": [float(v) for v in lam],
        "first": [float(v) for v in first],
        "last": [float(v) for v in last],
        "pair": np.stack([1.0 + 2.0 * same, cross], 1).astype(np.float32),
        "sine": sine.astype(np.float32),
        "wave": np.broadcast_to(wave, (blocks, LANES)).astype(np.float32).copy(),
    }


def call(body, outs, *args, smem=(), far=(), far_out=False, scratch=(), flops=1e9):
    specs = [
        pl.BlockSpec(memory_space=pltpu.SMEM if i in smem else pl.ANY if i in far else VMEM)
        for i in range(len(args))
    ]
    return pl.pallas_call(
        body,
        out_shape=[jax.ShapeDtypeStruct(s, f32) for s in outs],
        in_specs=specs,
        out_specs=[pl.BlockSpec(memory_space=pl.ANY if far_out else VMEM)] * len(outs),
        scratch_shapes=list(scratch),
        compiler_params=pltpu.CompilerParams(vmem_limit_bytes=16 * 2**20),
        cost_estimate=pl.CostEstimate(flops=int(flops), bytes_accessed=4 << 20, transcendentals=0),
    )(*args)


def row_roll(x, up):
    n = x.shape[0]
    if n % 8 == 0:
        return pltpu.roll(x, n - 1 if up else 1, 0)
    if up:
        return jnp.concatenate([x[1:], x[:1]], 0)
    return jnp.concatenate([x[-1:], x[:-1]], 0)


def lane_roll(x, up):
    n = x.shape[1]
    return pltpu.roll(x, n - 1 if up else 1, 1)


def fold_lanes(x):
    total = x[:, :LANES]
    for i in range(1, x.shape[1] // LANES):
        total = total + x[:, i * LANES : (i + 1) * LANES]
    return jnp.sum(total, axis=0, keepdims=True)


def smear_blocks(smear, size):
    n = smear.shape[0]
    i = lax.broadcasted_iota(jnp.int32, (n, size), 0)
    j = lax.broadcasted_iota(jnp.int32, (n, size), 1)
    wide_pick = jnp.where(i == j % n, 1.0, 0.0)
    i = lax.broadcasted_iota(jnp.int32, (size, n), 0)
    j = lax.broadcasted_iota(jnp.int32, (size, n), 1)
    tall_pick = jnp.where(i % n == j, 1.0, 0.0)
    tiled = mat(tall_pick, mat(smear, wide_pick))
    i = lax.broadcasted_iota(jnp.int32, (size, size), 0)
    j = lax.broadcasted_iota(jnp.int32, (size, size), 1)
    return jnp.where(i // n == j // n, tiled, 0.0)


def conducted(t, p, pairs):
    flux = jnp.zeros_like(t)
    faces = jnp.zeros_like(t)
    for near_t, near_p in pairs:
        differ = near_p != p
        flux = flux + jnp.where(differ, -2.0 * t, near_t - t)
        faces = faces + jnp.where(differ, 1.0, 0.0)
    k = jnp.where(p > 0.5, conduct_liquid, conduct_vapor)
    value = t + diffusion * k * flux
    return value, 2.0 * k * faces * value


def heat_body(dims, inner, *refs):
    thick, north, span, size_y, size_x, most = dims
    if inner:
        (table, temp, phase, ylo, yhi, smear, smear_e, heated, source, mob, pp, mass, mask) = refs
        tp = temp
    else:
        (table, temp, phase, zlo, zhi, ylo, yhi, smear, smear_e,
         heated, source, tp, pp, mass, mask) = refs
    skip = 1 if inner else 0
    base = 1 - skip
    planes = thick - 2 * skip
    tiles_y = north // size_y
    tiles_x = span // size_x
    w, n = lax.axis_index("wide"), lax.axis_index("narrow")
    n_first, n_last = n == 0, n == lax.axis_size("narrow") - 1
    for z in range(thick):
        pp[z + base] = phase[z].astype(f32)
        if inner:
            mob[z] = jnp.where(pp[z] > 0.5, mobility_liquid, mobility_vapor)
        else:
            tp[z + 1] = temp[z]
    if not inner:
        w_first, w_last = w == 0, w == lax.axis_size("wide") - 1
        tp[0] = jnp.where(w_first, temp[0], zlo[0])
        pp[0] = jnp.where(w_first, phase[0].astype(f32), zlo[1])
        tp[thick + 1] = jnp.where(w_last, temp[thick - 1], zhi[0])
        pp[thick + 1] = jnp.where(w_last, phase[thick - 1].astype(f32), zhi[1])
    row = lax.broadcasted_iota(jnp.int32, (tiles_y, span), 0)
    lane = lax.broadcasted_iota(jnp.int32, (tiles_y, span), 1)
    tile = row * tiles_x + lane // size_x
    hit = tile == table[0]
    for i in range(1, most):
        hit = jnp.logical_or(hit, tile == table[i])
    mask[...] = jnp.where(hit, expansion, 0.0)
    r = lax.broadcasted_iota(jnp.int32, (size_y, span), 0)
    c = lax.broadcasted_iota(jnp.int32, (size_y, span), 1)

    def plane(z):
        for yc in range(tiles_y):
            at = pl.ds(yc * size_y, size_y)
            t = tp[z + base, at, :]
            p = pp[z + base, at, :]

            def edge(ref, halo, k, y, wall, own):
                if 0 <= y < north:
                    return ref[z + base, pl.ds(y, 1), :]
                return jnp.where(wall, own, halo[k, z])

            pairs = [
                (tp[z + base - 1, at, :], pp[z + base - 1, at, :]),
                (tp[z + base + 1, at, :], pp[z + base + 1, at, :]),
                (jnp.where(c == span - 1, t, lane_roll(t, True)),
                 jnp.where(c == span - 1, p, lane_roll(p, True))),
                (jnp.where(c == 0, t, lane_roll(t, False)),
                 jnp.where(c == 0, p, lane_roll(p, False))),
            ]
            y = (yc + 1) * size_y
            pairs.append((
                jnp.where(r == size_y - 1, edge(tp, yhi, 0, y, n_last, t[size_y - 1:]), row_roll(t, True)),
                jnp.where(r == size_y - 1, edge(pp, yhi, 1, y, n_last, p[size_y - 1:]), row_roll(p, True)),
            ))
            y = yc * size_y - 1
            pairs.append((
                jnp.where(r == 0, edge(tp, ylo, 0, y, n_first, t[:1]), row_roll(t, False)),
                jnp.where(r == 0, edge(pp, ylo, 1, y, n_first, p[:1]), row_roll(p, False)),
            ))
            value, vapor = conducted(t, p, pairs)
            heated[z - skip, at, :] = value
            to = pl.ds(pl.multiple_of((z - skip) * north, north) + yc * size_y, size_y)
            mass[to, :] = vapor

    lax.fori_loop(skip, thick - skip, lambda z, carry: (plane(z), carry)[1], 0)
    smear_n = smear_blocks(smear[...], north)
    for tx in range(tiles_x):
        at = slice(tx * size_x, (tx + 1) * size_x)
        mass[:, at] = mat_t(mass[:, at], smear_e[...])
    for z in range(planes):
        smeared = mat(smear_n, mass[z * north : (z + 1) * north, :])
        for yc in range(tiles_y):
            part = smeared[yc * size_y : (yc + 1) * size_y] * mask[yc : yc + 1, :]
            if inner:
                source[z, yc * size_y : (yc + 1) * size_y, :] = part
            else:
                source[yc, z] = part


def pack_body(dims, listing, far_temp, far_phase, out, side_first, side_last, temp, phase, entry, sems):
    wide, thick, rows, span, most = dims
    tiles = span // LANES
    per = thick * tiles * rows
    north = wide * rows
    copies = [
        pltpu.make_async_copy(far_temp, temp, sems.at[0]),
        pltpu.make_async_copy(far_phase, phase, sems.at[1]),
    ]
    for copy in copies:
        copy.start()
    entry[...] = jnp.full((8, LANES), -1.0, f32)
    entry[0:1, 0:most] = listing[0].astype(f32)
    odd = lax.axis_index("narrow") % 2 == 1
    for w in range(wide):
        out[w, 2 * per :, :] = entry[...]
    for a, ref in enumerate((temp, phase)):
        copies[a].wait()
        for z in range(thick):
            side_first[a, z] = ref[z, 0:1, :].astype(f32)
            side_last[a, z] = ref[z, north - 1 : north, :].astype(f32)
            for w in range(wide):
                for t in range(tiles):
                    at = a * per + (z * tiles + t) * rows
                    piece = ref[z, w * rows : (w + 1) * rows, t * LANES : (t + 1) * LANES]
                    out[jnp.where(odd, wide - 1 - w, w), at : at + rows, :] = piece.astype(f32)


def edge_body(dims, lam, got, shift, first, last, scale):
    half = shift.shape[0] // 2
    for parity in range(2):
        mu = shift[parity * half : (parity + 1) * half, :]
        for ky, value in enumerate(lam):
            at = (parity * len(lam) + ky) * half
            scale[at : at + half, :] = 1.0 / (mu + value)
    wide, thick, rows, span, _ = dims
    tiles = span // LANES
    per = thick * tiles * rows
    for a in range(2):
        for w in range(wide):
            for z in range(thick):
                for t in range(tiles):
                    at = a * per + (z * tiles + t) * rows
                    row = a * wide * thick + w * thick + z
                    lanes = slice(t * LANES, (t + 1) * LANES)
                    first[row : row + 1, lanes] = got[w, at : at + 1, :]
                    last[row : row + 1, lanes] = got[w, at + rows - 1 : at + rows, :]


def boil_body(dims, tab, got, lo, hi, smear, smear_e, fwd, c_x, shift,
              source, mob, mob_lo, mob_hi, spec, message, outer, tp, pp, mass, heated, mask, entries):
    wide, thick, rows, span, _ = dims
    depth = wide * thick
    tiles = span // LANES
    per = thick * tiles * rows
    size_x = smear_e.shape[0]
    w, n = lax.axis_index("wide"), lax.axis_index("narrow")
    chunk = jnp.where(n % 2 == 1, wide - 1 - w, w)
    own = n * wide + chunk
    for w in range(wide):
        entries[w : w + 1, :] = got[w, 2 * per : 2 * per + 1, :]
        for z in range(thick):
            for t in range(tiles):
                at = (z * tiles + t) * rows
                to = ((w * thick + z) * rows, t * LANES)
                to = (slice(to[0], to[0] + rows), slice(to[1], to[1] + LANES))
                tp[to] = got[w, at : at + rows, :]
                pp[to] = got[w, per + at : per + at + rows, :]
    for tx in range(span // size_x):
        tile = (chunk * (span // size_x) + tx).astype(f32)
        hit = jnp.where(entries[...] == tile, expansion, 0.0)
        hit = jnp.max(hit, axis=1, keepdims=True)
        mask[:, tx * size_x : (tx + 1) * size_x] = jnp.broadcast_to(hit, (wide, size_x))
    mob[...] = jnp.where(pp[...] > 0.5, mobility_liquid, mobility_vapor)
    mob_lo[...] = jnp.where(lo[depth:, :] > 0.5, mobility_liquid, mobility_vapor)
    mob_hi[...] = jnp.where(hi[depth:, :] > 0.5, mobility_liquid, mobility_vapor)
    r = lax.broadcasted_iota(jnp.int32, (rows, span), 0)
    c = lax.broadcasted_iota(jnp.int32, (rows, span), 1)
    no_lo, no_hi = own == 0, own == lax.axis_size("narrow") * wide - 1

    def at_z(z):
        return pl.ds(pl.multiple_of(z * rows, rows), rows)

    def slab(z):
        t, p = tp[at_z(z), :], pp[at_z(z), :]
        below, above = at_z(jnp.maximum(z - 1, 0)), at_z(jnp.minimum(z + 1, depth - 1))

        def along_y(x, k, up):
            if up:
                edge = jnp.where(no_hi, x[rows - 1 :], hi[pl.ds(k * depth + z, 1), :])
                return jnp.where(r == rows - 1, edge, row_roll(x, True))
            edge = jnp.where(no_lo, x[:1], lo[pl.ds(k * depth + z, 1), :])
            return jnp.where(r == 0, edge, row_roll(x, False))

        pairs = [
            (tp[below, :], pp[below, :]),
            (tp[above, :], pp[above, :]),
            (along_y(t, 0, True), along_y(p, 1, True)),
            (along_y(t, 0, False), along_y(p, 1, False)),
            (jnp.where(c == span - 1, t, lane_roll(t, True)),
             jnp.where(c == span - 1, p, lane_roll(p, True))),
            (jnp.where(c == 0, t, lane_roll(t, False)),
             jnp.where(c == 0, p, lane_roll(p, False))),
        ]
        heated[at_z(z), :], mass[at_z(z), :] = conducted(t, p, pairs)

    lax.fori_loop(0, depth, lambda z, carry: (slab(z), carry)[1], 0)
    for w in range(wide):
        for k, z in enumerate((w * thick, (w + 1) * thick - 1)):
            outer[w, k * rows : (k + 1) * rows, :] = heated[z * rows : (z + 1) * rows, :]
    for tx in range(span // size_x):
        at = slice(tx * size_x, (tx + 1) * size_x)
        mass[:, at] = mat_t(mass[:, at], smear_e[...])
    group = LANES
    smear_n = smear_blocks(smear[...], group)
    for g in range(depth * rows // group):
        smeared = mat(smear_n, mass[g * group : (g + 1) * group, :])
        for i in range(group // rows):
            z = g * (group // rows) + i
            source[z * rows : (z + 1) * rows, :] = (
                smeared[i * rows : (i + 1) * rows] * mask[z // thick : z // thick + 1, :]
            )
    forward_body(
        (depth, rows, span), tab, source, mass, spec, fwd, c_x, shift, message,
        jnp.zeros((1, LANES), f32),
    )


def finish_body(dims, rho, parts, p, r, d, image, *refs):
    outer, out = refs if len(refs) == 2 else (None, refs[0])
    wide, thick, rows, span, _ = dims
    total = parts[0]
    for i in range(1, parts.shape[0]):
        total = total + parts[i]
    alpha = (rho[...] / jnp.sum(total, axis=1, keepdims=True))[:, :1]
    n = thick * rows
    tiles = span // LANES
    for w in range(wide):
        at = slice(w * n, (w + 1) * n)
        pressure = p[at, :] + alpha * d[at, :]
        residual = r[at, :] - alpha * image[at, :]
        if outer is None:
            out[w, :n, :] = pressure
            out[w, n : 2 * n, :] = residual
            continue
        units = [pressure[z * rows : (z + 1) * rows] for z in range(thick)]
        units += [residual[z * rows : (z + 1) * rows] for z in (0, thick - 1)]
        units += [outer[w, :rows, :], outer[w, rows:, :]]
        for u, unit in enumerate(units):
            for t in range(tiles):
                to = (u * tiles + t) * rows
                out[w, to : to + rows, :] = unit[:, t * LANES : (t + 1) * LANES]
        to = len(units) * tiles * rows
        for z in range(1, thick - 1):
            for y in (z * rows, (z + 1) * rows - 1):
                for t in range(tiles):
                    out[w, to : to + 1, :] = residual[y : y + 1, t * LANES : (t + 1) * LANES]
                    to += 1


def spread_body(dims, got, pressure, residual):
    wide, thick, rows, _, _ = dims
    for k, out in enumerate((pressure, residual)):
        for z in range(thick):
            row = (k * thick + z) * rows
            for w in range(wide):
                out[z, w * rows : (w + 1) * rows, :] = got[w, row : row + rows, :]


def gather_body(dims, got, inner, source, mob, *refs):
    wide, thick, rows, span, _ = dims
    tiles = span // LANES
    north = wide * rows
    pressure, residual, heated = refs[3:6]
    copies = [pltpu.make_async_copy(refs[3 + i], refs[i], refs[6].at[i]) for i in range(3)]
    odd = lax.axis_index("narrow") % 2 == 1
    planes = [(pressure, z) for z in range(thick)]
    planes += [(out, z) for out in (residual, heated) for z in (0, thick - 1)]
    for w in range(wide):
        chunk = jnp.where(odd, wide - 1 - w, w)
        y = pl.ds(pl.multiple_of(chunk * rows, rows), rows)
        for u, (out, z) in enumerate(planes):
            for t in range(tiles):
                at = (u * tiles + t) * rows
                out[z, y, t * LANES : (t + 1) * LANES] = got[w, at : at + rows, :]
    for z in range(1, thick - 1):
        heated[z] = inner[z - 1]
    copies[0].start()
    copies[2].start()
    r = lax.broadcasted_iota(jnp.int32, (rows, span), 0)
    c = lax.broadcasted_iota(jnp.int32, (rows, span), 1)
    for z in range(1, thick - 1):

        def part(i, z=z):
            start = pl.multiple_of(i * rows, rows)
            at = pl.ds(start, rows)
            v, b = pressure[z, at, :], mob[z, at, :]
            flux = jnp.where(c == span - 1, 0.0, (b + lane_roll(b, True)) * (v - lane_roll(v, True)))
            total = flux - lane_roll(flux, False)
            for k in (z - 1, z + 1):
                total = total + (b + mob[k, at, :]) * (v - pressure[k, at, :])
            y = jnp.minimum(start + rows, north - 1)
            v_hi = jnp.where(r == rows - 1, pressure[z, pl.ds(y, 1), :], row_roll(v, True))
            b_hi = jnp.where(r == rows - 1, mob[z, pl.ds(y, 1), :], row_roll(b, True))
            y = jnp.maximum(start - 1, 0)
            v_lo = jnp.where(r == 0, pressure[z, pl.ds(y, 1), :], row_roll(v, False))
            b_lo = jnp.where(r == 0, mob[z, pl.ds(y, 1), :], row_roll(b, False))
            total = total + (b + b_hi) * (v - v_hi) + (b + b_lo) * (v - v_lo)
            residual[z, at, :] = source[z - 1, at, :] - (compress * v + 0.5 * total)

        lax.fori_loop(0, wide, lambda i, carry: (part(i), carry)[1], 0)
        first = len(planes) * tiles * rows + (z - 1) * 2 * tiles
        for side, y in enumerate((0, north - 1)):
            lower = 0 if side == 0 else wide - 1
            w = jnp.where(odd, wide - 1 - lower, lower)
            for t in range(tiles):
                at = first + side * tiles + t
                residual[z, y : y + 1, t * LANES : (t + 1) * LANES] = got[w, at : at + 1, :]
    copies[1].start()
    for copy in copies:
        copy.wait()


def forward_body(dims, tab, field, fold, spec, fwd, c_x, shift, message, extra):
    depth, rows, span = dims
    half = depth // 2
    size = half * rows
    for parity in range(2):
        for z in range(half):
            a = field[z * rows : (z + 1) * rows, :]
            b = field[(depth - 1 - z) * rows : (depth - z) * rows, :]
            fold[z * rows : (z + 1) * rows, :] = a + b if parity == 0 else a - b
        spec[parity * size : (parity + 1) * size, :] = mat_t(
            mat(fwd[parity], fold[:size, :]), c_x[...]
        )
    for parity in range(2):
        low = jnp.zeros((half, span), f32)
        high = jnp.zeros((half, span), f32)
        for ky in range(rows):
            at = parity * size + ky * half
            g = spec[at : at + half, :] * shift[at : at + half, :]
            low = low + tab["first"][ky] * g
            high = high + tab["last"][ky] * g
        for k in range(half):
            o = parity * half + k
            message[o, 0:1, :span] = low[k : k + 1]
            message[o, 0:1, span : 2 * span] = high[k : k + 1]
            message[o, 0:1, 2 * span :] = extra


def start_body(dims, tab, source, fwd, c_x, shift, spec, message, fold):
    forward_body(dims, tab, source, fold, spec, fwd, c_x, shift, message, jnp.zeros((1, LANES), f32))


def solve_body(dims, first_call, seats, *refs):
    depth, rows, span = dims
    half = depth // 2
    if first_call:
        (got, spec, shift, pairs, sine, wave, h_new, message, low, high) = refs
    else:
        (got, spec, shift, pairs, sine, wave, image_spec, h_old, rho,
         spec_new, h_new, message, alpha_out, low, high) = refs
    pair = pairs[lax.axis_index("narrow") * lax.axis_size("wide") + lax.axis_index("wide")]
    blocks = len(seats)
    for j, i in enumerate(seats):
        low[j : j + 1, :] = got[i, 0:1, :span]
        high[j : j + 1, :] = got[i, 0:1, span : 2 * span]
    jump = high[...] - row_roll(low[...], True)
    r = lax.broadcasted_iota(jnp.int32, (blocks, span), 0)
    jump = jnp.where(r == blocks - 1, 0.0, jump)
    if not first_call:
        bottom = jnp.zeros((1, LANES), f32)
        for j in range(blocks):
            bottom = bottom + got[j, 0:1, 2 * span :]
        alpha = rho[...] / jnp.sum(bottom, axis=1, keepdims=True)
        alpha_out[...] = alpha
        alpha = alpha[:, :1]
        jump = h_old[...] - alpha * jump
    h_new[...] = jump
    scale = 1.0 / (pair[0:1, :] - wave[:, :1] * pair[1:2, :])
    q = mat(sine[...], mat(sine[...], jump) * scale)
    total = fold_lanes(q * jump) * -1.0
    acc = jnp.zeros((8, span), f32)
    for parity in range(2):
        for ky in range(rows):
            at = parity * half * rows + ky * half
            s = spec[at : at + half, :]
            if not first_call:
                s = s - alpha * image_spec[at : at + half, :]
                spec_new[at : at + half, :] = s
            e = s * s * shift[at : at + half, :]
            for i in range(half // 8):
                acc = acc + e[i * 8 : (i + 1) * 8]
    total = total + fold_lanes(acc)
    zero = jnp.zeros((1, span), f32)
    for j, i in enumerate(seats):
        message[i, 0:1, :span] = zero if j == 0 else q[j - 1 : j]
        message[i, 0:1, span : 2 * span] = q[j : j + 1]
        message[i, 0:1, 2 * span :] = total


def advance_body(dims, tab, first_call, last_call, blocks, *refs):
    depth, rows, span = dims
    half = depth // 2
    size = half * rows
    refs = list(refs)
    take = refs.pop
    if last_call:
        n = ITERS - 1
        at = 13
        refs[at : at + 3 * n] = [refs[at : at + n], refs[at + n : at + 2 * n], refs[at + 2 * n : at + 3 * n]]
    got, spec, shift, inv, fwd, c_x, swap, mob, mob_lo, mob_hi = [take(0) for _ in range(10)]
    if not first_call:
        dir_old, q_old, rho_old = [take(0) for _ in range(3)]
    if last_call:
        alphas, olds, images, source = take(0), take(0), take(0), take(0)
    direction, image = take(0), take(0)
    if last_call:
        rho_out, part_out, p_out, r_out = [take(0) for _ in range(4)]
    else:
        rho_out, dir_spec, q_out, image_spec, message = [take(0) for _ in range(5)]
    work, q_mid, fold = take(0), take(0), take(0)
    if last_call:
        dir_spec, q_out = take(0), take(0)

    total = jnp.zeros((1, LANES), f32)
    for o in range(depth):
        q_mid[o : o + 1, :] = got[o, 0:1, :span]
        q_mid[depth + o : depth + o + 1, :] = got[o, 0:1, span : 2 * span]
        total = total + got[o, 0:1, 2 * span :]
    rho = jnp.sum(total, axis=1, keepdims=True) + jnp.zeros((1, LANES), f32)
    rho_out[...] = rho
    if not first_call:
        beta = (rho / rho_old[...])[:, :1]
    for parity in range(2):
        at_q = parity * half
        q_lo = q_mid[at_q : at_q + half, :]
        q_hi = q_mid[depth + at_q : depth + at_q + half, :]
        for ky in range(rows):
            at = parity * size + ky * half
            u = (spec[at : at + half, :] + tab["first"][ky] * q_lo - tab["last"][ky] * q_hi) * (
                shift[at : at + half, :]
            )
            if not first_call:
                u = u + beta * dir_old[at : at + half, :]
            dir_spec[at : at + half, :] = u
    q = q_mid[...]
    if not first_call:
        q = q + beta * q_old[...]
    q_out[...] = q
    q_mid[...] = mat(swap[...], mat(q, c_x[...]))
    for parity in range(2):
        fold[parity * size : (parity + 1) * size, :] = mat(
            inv[parity], mat(dir_spec[parity * size : (parity + 1) * size, :], c_x[...])
        )
    for z in range(half):
        a = fold[z * rows : (z + 1) * rows, :]
        b = fold[size + z * rows : size + (z + 1) * rows, :]
        direction[z * rows : (z + 1) * rows, :] = a + b
        direction[(depth - 1 - z) * rows : (depth - z) * rows, :] = a - b

    r = lax.broadcasted_iota(jnp.int32, (rows, span), 0)
    c = lax.broadcasted_iota(jnp.int32, (rows, span), 1)
    acc = jnp.zeros((1, span), f32)
    below = None
    for z in range(depth):
        at = slice(z * rows, (z + 1) * rows)
        v = direction[at, :]
        b = mob[at, :]
        out = compress * v
        flux = jnp.where(c == span - 1, 0.0, (b + lane_roll(b, True)) * (v - lane_roll(v, True)))
        out_flux = flux - lane_roll(flux, False)
        b_hi = b[rows - 1 :] + mob_hi[z : z + 1, :]
        flux = jnp.where(
            r == rows - 1,
            b_hi * q_mid[depth + z : depth + z + 1, :],
            (b + row_roll(b, True)) * (v - row_roll(v, True)),
        )
        f_lo = (b[:1] + mob_lo[z : z + 1, :]) * q_mid[z : z + 1, :]
        out_flux = out_flux + flux - jnp.where(r == 0, f_lo, row_roll(flux, False))
        if below is not None:
            out_flux = out_flux - below
        if z + 1 < depth:
            up = slice((z + 1) * rows, (z + 2) * rows)
            below = (b + mob[up, :]) * (v - direction[up, :])
            out_flux = out_flux + below
        out = out + 0.5 * out_flux
        image[at, :] = out
        acc = acc + jnp.sum(v * out, axis=0, keepdims=True)
    part = fold_lanes(acc)
    if last_call:
        for i in range(blocks):
            part_out[i] = part
        p = alphas[0][:, :1] * olds[0][...]
        r = source[...] - alphas[0][:, :1] * images[0][...]
        for i in range(1, len(olds)):
            p = p + alphas[i][:, :1] * olds[i][...]
            r = r - alphas[i][:, :1] * images[i][...]
        p_out[...] = p
        r_out[...] = r
    else:
        forward_body(dims, tab, image, work, image_spec, fwd, c_x, shift, message, part)


def split_by_z(superheat_excess, liquid_indicator, listing, smear_n, smear_e, dims, const):
    thick, north, span = superheat_excess.shape
    wide, lanes = lax.axis_size("wide"), lax.axis_size("narrow")
    depth, rows, span = dims[1]
    size_y, size_x = smear_n.shape[0], smear_e.shape[0]
    tiles_y = north // size_y
    whole = depth * rows
    phase = liquid_indicator.astype(f32)
    both = jnp.stack([superheat_excess, phase])
    up = [(i, i + 1) for i in range(wide - 1)]
    down = [(i + 1, i) for i in range(wide - 1)]
    zlo = lax.ppermute(both[:, thick - 1], "wide", up)
    zhi = lax.ppermute(both[:, 0], "wide", down)
    up = [(i, i + 1) for i in range(lanes - 1)]
    down = [(i + 1, i) for i in range(lanes - 1)]
    ylo = lax.ppermute(both[:, :, north - 1 :], "narrow", up)
    yhi = lax.ppermute(both[:, :, :1], "narrow", down)

    def regroup(x):
        x = x.reshape(wide, thick * rows, span)
        return lax.all_to_all(x, "wide", split_axis=0, concat_axis=0, tiled=True)

    mob = jnp.where(phase > 0.5, mobility_liquid, mobility_vapor)
    mob = mob.reshape(thick, wide, rows, span).transpose(1, 0, 2, 3)
    mob = regroup(mob).reshape(depth, rows, span)
    most = listing.size
    heat_dims = (thick, north, span, size_y, size_x, most)
    heated, source = call(
        lambda *r: heat_body(heat_dims, False, *r),
        [(thick, north, span), (tiles_y, thick, size_y, span)],
        listing.reshape(-1), superheat_excess, liquid_indicator, zlo, zhi, ylo, yhi,
        smear_n, smear_e,
        smem=(0,),
        scratch=[
            VMEM((thick + 2, north, span), f32),
            VMEM((thick + 2, north, span), f32),
            VMEM((thick * north, span), f32),
            VMEM((tiles_y, span), f32),
        ],
    )
    source, mob = lax.optimization_barrier((source, mob))
    if size_y != rows:
        source = source.transpose(1, 0, 2, 3).reshape(thick, wide, rows, span).transpose(1, 0, 2, 3)
    source = regroup(source).reshape(whole, span)
    up, down = const["row_pairs"]
    mob_lo = lax.ppermute(mob[:, rows - 1], ("wide", "narrow"), up)
    mob_hi = lax.ppermute(mob[:, 0], ("wide", "narrow"), down)
    spec, message = call(
        lambda *r: start_body(dims[1], const["tab"], *r), [(whole, span), const["letter"]],
        source, const["forward"], const["c_x"], const["shift"],
        scratch=[VMEM((whole, span), f32)],
    )
    return heated, source, mob.reshape(whole, span), mob_lo, mob_hi, spec, message


def split_by_y(superheat_excess, liquid_indicator, listing, smear_n, smear_e, dims, const):
    depth, rows, span = dims[1]
    wide, thick = dims[0][:2]
    lanes = lax.axis_size("narrow")
    whole = depth * rows
    per = thick * rows * (span // LANES)
    north = superheat_excess.shape[1]
    packed, side_first, side_last = call(
        lambda *r: pack_body(dims[0], *r),
        [(wide, 2 * per + 8, LANES), (2, thick, 1, span), (2, thick, 1, span)],
        listing, superheat_excess, liquid_indicator, far=(1, 2),
        scratch=[
            VMEM((thick, north, span), f32),
            VMEM((thick, north, span), jnp.int32),
            VMEM((8, LANES), f32),
            pltpu.SemaphoreType.DMA((2,)),
        ],
    )
    got = lax.all_to_all(packed, "wide", split_axis=0, concat_axis=0, tiled=True)
    first, last, const["shift"] = call(
        lambda *r: edge_body(dims[0], const["tab"]["lam"], *r),
        [(2 * depth, span)] * 2 + [(whole, span)], got, const["shift"],
    )
    up, down = const["row_pairs"]
    lo = lax.ppermute(last, ("wide", "narrow"), up)
    hi = lax.ppermute(first, ("wide", "narrow"), down)
    full, plane = (whole, span), (depth, span)
    y_up = [(i, i + 1) for i in range(lanes - 1)]
    y_down = [(i + 1, i) for i in range(lanes - 1)]
    ylo = lax.ppermute(side_last, "narrow", y_up)
    yhi = lax.ppermute(side_first, "narrow", y_down)
    block, inner = (thick, north, span), (thick - 2, north, span)
    size_y, size_x = smear_n.shape[0], smear_e.shape[0]
    heat_dims = (thick, north, span, size_y, size_x, listing.size)
    middle = call(
        lambda *r: heat_body(heat_dims, True, *r),
        [inner, inner, block],
        listing.reshape(-1), superheat_excess, liquid_indicator, ylo, yhi, smear_n, smear_e,
        smem=(0,),
        scratch=[
            VMEM(block, f32),
            VMEM(((thick - 2) * north, span), f32),
            VMEM((north // size_y, span), f32),
        ],
    )
    lo, hi, *middle = lax.optimization_barrier((lo, hi, *middle))
    return middle, *call(
        lambda *r: boil_body(dims[0], const["tab"], *r),
        [full, full, plane, plane, full, const["letter"], (wide, 2 * rows, span)],
        got, lo, hi, smear_n, smear_e, const["forward"], const["c_x"], const["shift"],
        scratch=[VMEM(full, f32)] * 4 + [VMEM((wide, span), f32), VMEM((wide, LANES), f32)],
    )


def on_device(superheat_excess, liquid_indicator, listing, smear_n, smear_e):
    thick, north, span = superheat_excess.shape
    wide, lanes = lax.axis_size("wide"), lax.axis_size("narrow")
    blocks = wide * lanes
    depth = thick * wide
    rows = north // wide
    size_y = smear_n.shape[0]
    shape = (depth, rows, span)
    dims = ((wide, thick, rows, span, listing.size), shape)
    tab = tables(depth, rows, span, blocks)
    whole = depth * rows
    full, one = (whole, span), (1, LANES)
    letter = (blocks, 1, 2 * span + LANES)

    by_y = rows == size_y and thick > 2

    def seat(j):
        n, c = j // wide, j % wide
        return n, wide - 1 - c if by_y and n % 2 == 1 else c

    def place(j):
        n, w = seat(j)
        return w * lanes + n

    seats = [n * wide + w for n, w in map(seat, range(blocks))]
    up = [(place(j), place(j + 1)) for j in range(blocks - 1)]
    const = {k: jnp.asarray(tab[k]) for k in ("c_x", "forward", "inverse", "swap", "shift", "pair", "sine", "wave")}
    const["tab"], const["letter"] = tab, letter
    const["row_pairs"] = up, [(b, a) for a, b in up]
    if not by_y:
        mu = const["shift"].reshape(2, 1, depth // 2, span)
        lam = jnp.asarray(tab["lam"], f32).reshape(1, rows, 1, 1)
        const["shift"] = (1.0 / (mu + lam)).reshape(full)
    if by_y:
        middle, source, mob, mob_lo, mob_hi, spec, message, outer = split_by_y(
            superheat_excess, liquid_indicator, listing, smear_n, smear_e, dims, const
        )
    else:
        heated, source, mob, mob_lo, mob_hi, spec, message = split_by_z(
            superheat_excess, liquid_indicator, listing, smear_n, smear_e, dims, const
        )

    def swap_all(x):
        return lax.all_to_all(x, ORDER, split_axis=0, concat_axis=0, tiled=True)

    shift, pair, sine, wave = (const[k] for k in ("shift", "pair", "sine", "wave"))
    pair_scratch = [VMEM((blocks, span), f32)] * 2
    jump, message = call(
        lambda *r: solve_body(shape, True, seats, *r), [(blocks, span), letter],
        swap_all(message), spec, shift, pair, sine, wave, scratch=pair_scratch,
    )
    dir_spec = q = rho = None
    directions, images, alphas = [], [], []
    for iteration in range(ITERS):
        first, final = iteration == 0, iteration + 1 == ITERS
        args = [swap_all(message), spec, shift, const["inverse"], const["forward"], const["c_x"], const["swap"], mob, mob_lo, mob_hi]
        if not first:
            args += [dir_spec, q, rho]
        outs = [full, full, one]
        work = [VMEM(full, f32), VMEM((2 * depth, span), f32), VMEM(full, f32)]
        if final:
            outs += [(blocks, 1, LANES), full, full]
            args += [*alphas, *directions, *images, source]
            work += [VMEM(full, f32), VMEM((2 * depth, span), f32)]
        else:
            outs += [full, (2 * depth, span), full, letter]
        result = call(
            lambda *r, a=first, b=final: advance_body(shape, tab, a, b, blocks, *r), outs, *args,
            scratch=work,
        )
        directions.append(result[0])
        images.append(result[1])
        rho = result[2]
        if final:
            parts = swap_all(result[3])
            pressure, residual = result[4:]
        else:
            dir_spec, q, image_spec, message = result[3:]
            spec, jump, message, alpha = call(
                lambda *r: solve_body(shape, False, seats, *r),
                [full, (blocks, span), letter, one],
                swap_all(message), spec, shift, pair, sine, wave, image_spec, jump, rho,
                scratch=pair_scratch,
            )
            alphas.append(alpha)

    if by_y:
        extra = [outer]
        tiles = span // LANES
        lines = (thick + 4) * rows * tiles + -(-2 * (thick - 2) * tiles // 8) * 8
        packet = (wide, lines, LANES)
    else:
        extra = []
        packet = (wide, 2 * thick * rows, span)
    (both,) = call(
        lambda *r: finish_body(dims[0], *r), [packet],
        rho, parts, pressure, residual, directions[2], images[2], *extra,
    )
    both = lax.all_to_all(both, "wide", split_axis=0, concat_axis=0, tiled=True)
    block = (thick, north, span)
    if not by_y:
        pressure, residual = call(lambda *r: spread_body(dims[0], *r), [block] * 2, both)
        return heated, pressure, residual
    pressure, residual, heated = call(
        lambda *r: gather_body(dims[0], *r), [block] * 3, both, *middle, far_out=True,
        scratch=[VMEM(block, f32)] * 3 + [pltpu.SemaphoreType.DMA((3,))],
    )
    return heated, pressure, residual


def solution(mesh):
    spec = P("wide", "narrow", None)
    return jax.shard_map(
        on_device,
        mesh=mesh,
        in_specs=(spec, spec, spec, P(), P()),
        out_specs=(spec, spec, spec),
        check_vma=False,
    )
```
